32 devices in a mesh: tp: 4 (over z), cp: 8 (over y, x, core).
Axes of the slice: x: 2, y: 2, z: 4, core: 2. Of those that a mesh axis runs over, the one named last changes fastest.
Arguments:
- x_in: bfloat16 [8192, 2560], P('cp')
- positions: int32 [8192], P('cp')
- attn_gain: bfloat16 [2, 2560], replicated
- mlp_gain: bfloat16 [2, 2560], replicated
- w_query: bfloat16 [2, 2560, 2560], P(None, None, 'tp')
- b_query: bfloat16 [2, 2560], P(None, 'tp')
- w_key: bfloat16 [2, 2560, 2560], P(None, None, 'tp')
- b_key: bfloat16 [2, 2560], P(None, 'tp')
- w_value: bfloat16 [2, 2560, 2560], P(None, None, 'tp')
- b_value: bfloat16 [2, 2560], P(None, 'tp')
- w_out: bfloat16 [2, 2560, 2560], P(None, 'tp')
- w_gate: bfloat16 [2, 2560, 6912], P(None, None, 'tp')
- w_up: bfloat16 [2, 2560, 6912], P(None, None, 'tp')
- w_down: bfloat16 [2, 6912, 2560], P(None, 'tp')
Outputs:
- output 1: bfloat16 [8192, 2560], P('cp')
- output 2: bfloat16 [8192, 20, 128], P('cp', 'tp')
- output 3: bfloat16 [8192, 20, 128], P('cp', 'tp')
- output 4: bfloat16 [8192, 20, 128], P('cp', 'tp')
- output 5: bfloat16 [8192, 20, 128], P('cp', 'tp')
All inputs are finite; a program needn't handle non-finite values.
Results may differ from the reference program's by a relative error of at most 0.02.
Values are sent between devices in bfloat16 or wider.
A program may use at most 1 GiB of HBM per device.

```python
import jax
import jax.numpy as jnp
from jax import lax

TOKENS = 8192
HIDDEN = 2560
Q_HEADS = 20
KV_HEADS = 20
HEAD_DIM = 128
FFN_DIM = 6912
WINDOW = 4096


def setup_inputs(seed: int = 0) -> dict:
    key_list = jax.random.split(jax.random.key(seed), 14)
    q_width = Q_HEADS * HEAD_DIM
    kv_width = KV_HEADS * HEAD_DIM

    def normal_draw(key_idx, arr_shape, factor):
        return (jax.random.normal(key_list[key_idx], arr_shape, jnp.float32) * factor).astype(jnp.bfloat16)

    def gain_draw(key_idx):
        return jax.random.uniform(key_list[key_idx], (2, HIDDEN), jnp.float32, 0.5, 1.5).astype(jnp.bfloat16)

    pos_start = jax.random.randint(key_list[1], (), 0, 8192, jnp.int32)
    return {
        'x_in': normal_draw(0, (TOKENS, HIDDEN), 1.0),
        'positions': pos_start + jnp.arange(TOKENS, dtype=jnp.int32),
        'attn_gain': gain_draw(2),
        'mlp_gain': gain_draw(3),
        'w_query': normal_draw(4, (2, HIDDEN, q_width), 2.0 * HIDDEN ** -0.5),
        'b_query': normal_draw(5, (2, q_width), 0.5),
        'w_key': normal_draw(6, (2, HIDDEN, kv_width), 2.0 * HIDDEN ** -0.5),
        'b_key': normal_draw(7, (2, kv_width), 0.5),
        'w_value': normal_draw(8, (2, HIDDEN, kv_width), HIDDEN ** -0.5),
        'b_value': normal_draw(9, (2, kv_width), 0.5),
        'w_out': normal_draw(10, (2, q_width, HIDDEN), 2.0 * q_width ** -0.5),
        'w_gate': normal_draw(11, (2, HIDDEN, FFN_DIM), HIDDEN ** -0.5),
        'w_up': normal_draw(12, (2, HIDDEN, FFN_DIM), HIDDEN ** -0.5),
        'w_down': normal_draw(13, (2, FFN_DIM, HIDDEN), FFN_DIM ** -0.5),
    }


def rms_norm(hidden, gain):
    hidden_f = hidden.astype(jnp.float32)
    variance = jnp.mean(hidden_f * hidden_f, axis=-1, keepdims=True)
    return (hidden_f * lax.rsqrt(variance + 1e-6) * gain.astype(jnp.float32)).astype(jnp.bfloat16)


def rope_tables(positions):
    inv_freq = 1.0 / (1000000.0 ** (jnp.arange(0, HEAD_DIM, 2, dtype=jnp.float32) / HEAD_DIM))
    angles = positions.astype(jnp.float32)[:, None] * inv_freq[None, :]
    return jnp.cos(angles)[:, None, :], jnp.sin(angles)[:, None, :]


def apply_rope(proj_f, cos_tab, sin_tab):
    half_dim = proj_f.shape[-1] // 2
    first_half = proj_f[..., :half_dim]
    second_half = proj_f[..., half_dim:]
    return jnp.concatenate([first_half * cos_tab - second_half * sin_tab, second_half * cos_tab + first_half * sin_tab], axis=-1)


def project(normed, weight, bias_vec):
    return jnp.dot(normed, weight, preferred_element_type=jnp.float32) + bias_vec.astype(jnp.float32)


def attention(queries, key_cache, value_cache, window):
    group_size = Q_HEADS // KV_HEADS
    block_len = 128
    block_count = TOKENS // block_len
    q_blocks = queries.reshape(block_count, block_len, KV_HEADS, group_size, HEAD_DIM).astype(jnp.float32)
    keys_f = key_cache.astype(jnp.float32)
    values_f = value_cache.astype(jnp.float32)
    key_pos = jnp.arange(TOKENS)
    score_scale = HEAD_DIM ** -0.5

    def one_block(block_in):
        block_idx, q_blk = block_in
        query_pos = block_idx * block_len + jnp.arange(block_len)
        scores = jnp.einsum('qkgd,skd->qkgs', q_blk, keys_f) * score_scale
        allowed = (key_pos[None, :] <= query_pos[:, None]) & (key_pos[None, :] > query_pos[:, None] - window)
        scores = jnp.where(allowed[:, None, None, :], scores, -jnp.inf)
        probs = jax.nn.softmax(scores, axis=-1).astype(jnp.bfloat16).astype(jnp.float32)
        return jnp.einsum('qkgs,skd->qkgd', probs, values_f).astype(jnp.bfloat16)

    attn_out = lax.map(one_block, (jnp.arange(block_count), q_blocks))
    return attn_out.reshape(TOKENS, Q_HEADS * HEAD_DIM)


def reference(x_in, positions, attn_gain, mlp_gain, w_query, b_query, w_key, b_key, w_value, b_value, w_out, w_gate, w_up, w_down):
    cos_tab, sin_tab = rope_tables(positions)
    hidden = x_in
    caches = []
    for layer_idx, window in ((0, TOKENS), (1, WINDOW)):
        normed = rms_norm(hidden, attn_gain[layer_idx])
        queries = apply_rope(project(normed, w_query[layer_idx], b_query[layer_idx]).reshape(TOKENS, Q_HEADS, HEAD_DIM), cos_tab, sin_tab).astype(jnp.bfloat16)
        key_cache = apply_rope(project(normed, w_key[layer_idx], b_key[layer_idx]).reshape(TOKENS, KV_HEADS, HEAD_DIM), cos_tab, sin_tab).astype(jnp.bfloat16)
        value_cache = project(normed, w_value[layer_idx], b_value[layer_idx]).astype(jnp.bfloat16).reshape(TOKENS, KV_HEADS, HEAD_DIM)
        attn_out = attention(queries, key_cache, value_cache, window)
        hidden = (hidden.astype(jnp.float32) + jnp.dot(attn_out, w_out[layer_idx], preferred_element_type=jnp.float32)).astype(jnp.bfloat16)
        normed = rms_norm(hidden, mlp_gain[layer_idx])
        gate_proj = jnp.dot(normed, w_gate[layer_idx], preferred_element_type=jnp.float32)
        up_proj = jnp.dot(normed, w_up[layer_idx], preferred_element_type=jnp.float32)
        activated = (jax.nn.silu(gate_proj) * up_proj).astype(jnp.bfloat16)
        hidden = (hidden.astype(jnp.float32) + jnp.dot(activated, w_down[layer_idx], preferred_element_type=jnp.float32)).astype(jnp.bfloat16)
        caches.append(key_cache)
        caches.append(value_cache)
    return (hidden, caches[0], caches[1], caches[2], caches[3])
```

```python
import functools

import jax
import jax.numpy as jnp
from jax import lax
from jax.experimental import pallas as pl
from jax.experimental.pallas import tpu as pltpu
from jax.sharding import PartitionSpec as P

MESH = pl.DeviceIdType.MESH
BF16 = jnp.bfloat16
F32 = jnp.float32
HEAD_DIM = 128
HEADS = 5
BLOCK = 1024
WIDTH = 2560
FFN = 1728
QKV = 3 * HEADS * HEAD_DIM
WINDOW_BLOCKS = 4
CHUNK = 256
PIECE = 64
TILE_Q = 512
EXP_SCALE = HEAD_DIM ** -0.5 * 1.4426950408889634
VMEM_LIMIT = 62 * 2 ** 20


def hbm():
    return pl.BlockSpec(memory_space=pl.ANY)


def vmem():
    return pl.BlockSpec(memory_space=pltpu.VMEM)


def normalize(rows, gain):
    rows_f = rows.astype(F32)
    variance = jnp.mean(rows_f * rows_f, axis=-1, keepdims=True)
    return (rows_f * lax.rsqrt(variance + 1e-6) * gain).astype(BF16)


def qkv_kernel(layer, x_ref, gain_ref, wq_ref, wk_ref, wv_ref, bias_ref, cos_ref, sin_ref,
               q_ref, k_ref, vt_ref, kout_ref, vout_ref, w_buf, sems):
    half = HEADS * HEAD_DIM
    loads = []
    for i, w in enumerate((wq_ref, wk_ref, wv_ref)):
        copy = pltpu.make_async_copy(w.at[layer], w_buf.at[i], sems.at[i])
        copy.start()
        loads.append(copy)
    gain = gain_ref[layer:layer + 1, :].astype(F32)
    for copy in loads:
        copy.wait()

    def chunk(j, _):
        rows = pl.ds(pl.multiple_of(j * CHUNK, CHUNK), CHUNK)
        normed = normalize(x_ref[rows, :], gain)
        cos = cos_ref[rows, :]
        sin = sin_ref[rows, :]
        for i in range(3):
            proj = jnp.dot(normed, w_buf[i], preferred_element_type=F32) + bias_ref[i:i + 1, :].astype(F32)
            for h in range(HEADS):
                part = proj[:, h * HEAD_DIM:(h + 1) * HEAD_DIM]
                cols = slice(h * HEAD_DIM, (h + 1) * HEAD_DIM)
                if i < 2:
                    part = (part * cos + pltpu.roll(part, HEAD_DIM // 2, 1) * sin).astype(BF16)
                if i == 0:
                    q_ref[h, rows, :] = part
                elif i == 1:
                    k_ref[h, rows, :] = part
                    kout_ref[rows, cols] = part
                else:
                    vout_ref[rows, cols] = part.astype(BF16)
                    vt_ref[h, :, rows] = part.T.astype(BF16)
        return 0

    lax.fori_loop(0, BLOCK // CHUNK, chunk, 0)


def qkv_call(layer, x, gain, wq, wk, wv, bias, cos, sin):
    shape = jax.ShapeDtypeStruct
    return pl.pallas_call(
        functools.partial(qkv_kernel, layer),
        out_shape=(
            shape((HEADS, BLOCK, HEAD_DIM), BF16),
            shape((HEADS, BLOCK, HEAD_DIM), BF16),
            shape((HEADS, HEAD_DIM, BLOCK), BF16),
            shape((BLOCK, HEADS * HEAD_DIM), BF16),
            shape((BLOCK, HEADS * HEAD_DIM), BF16),
        ),
        in_specs=[vmem(), vmem(), hbm(), hbm(), hbm(), vmem(), vmem(), vmem()],
        out_specs=(vmem(),) * 5,
        scratch_shapes=[
            pltpu.VMEM((3, WIDTH, HEADS * HEAD_DIM), BF16),
            pltpu.SemaphoreType.DMA((3,)),
        ],
        compiler_params=pltpu.CompilerParams(vmem_limit_bytes=VMEM_LIMIT),
        cost_estimate=pl.CostEstimate(flops=2 * BLOCK * WIDTH * QKV, bytes_accessed=20_000_000, transcendentals=0),
        name=f"qkv{layer}",
    )(x, gain, wq, wk, wv, bias, cos, sin)


def dot_rows(a, b):
    return lax.dot_general(a, b, (((1,), (1,)), ((), ())), preferred_element_type=F32)


def attention_kernel(windowed, q_ref, k_ref, vt_ref, o_ref, k_buf, v_buf, o_buf, m_s, l_s, a_s, s0, s1,
                     load_sem, send_sem, recv_sem, o_send, o_recv, o_local):
    z = lax.axis_index("tp")
    cp = lax.axis_index("cp")
    x_dev = cp + 2 - 4 * ((cp // 2) % 2)
    y_dev = cp + 4 - 8 * (cp // 4)
    c_dev = cp + 1 - 2 * (cp % 2)
    d_blk = x_dev + 4 - 8 * (x_dev // 4)

    barrier = pltpu.get_barrier_semaphore()
    for other in (x_dev, y_dev, c_dev):
        pl.semaphore_signal(barrier, inc=1, device_id=(z, other), device_id_type=MESH)
    for step in range(1, 4):
        pl.semaphore_signal(barrier, inc=1, device_id=(lax.rem(z + step, 4), cp), device_id_type=MESH)

    def load(h, which):
        src, dst = ((k_ref, k_buf), (vt_ref, v_buf))[which]
        return pltpu.make_async_copy(src.at[h], dst.at[h, cp], load_sem.at[h, which])

    for h in range(HEADS):
        load(h, 0).start()
        load(h, 1).start()
    pl.semaphore_wait(barrier, 6)

    def hop(h, slot, which, src_block, dev):
        buf = (k_buf, v_buf)[which]
        if src_block is None:
            src = (k_ref, vt_ref)[which].at[h]
            dst = buf.at[h, cp]
        else:
            src = buf.at[h, src_block]
            dst = buf.at[h, src_block]
        return pltpu.make_async_remote_copy(
            src_ref=src, dst_ref=dst, send_sem=send_sem.at[h, slot], recv_sem=recv_sem.at[h, slot],
            device_id=(z, dev), device_id_type=MESH)

    def own(h, action):
        for which in range(2):
            for slot, dev in ((0, x_dev), (2, y_dev), (4, c_dev)):
                action(hop(h, slot + which, which, None, dev))

    def forward_x(h, action):
        action(hop(h, 6, 0, x_dev, y_dev))
        action(hop(h, 8, 0, x_dev, c_dev))
        action(hop(h, 9, 1, x_dev, c_dev))

    def forward_y(h, action):
        action(hop(h, 7, 1, y_dev, x_dev))
        action(hop(h, 10, 0, y_dev, c_dev))
        action(hop(h, 11, 1, y_dev, c_dev))

    def start(copy):
        copy.start()

    def wait_send(copy):
        copy.wait_send()

    def received(h, slot, which, block):
        hop(h, slot, which, block, c_dev).wait_recv()

    def event_neighbours(h):
        received(h, 0, 0, x_dev)
        received(h, 1, 1, x_dev)
        forward_x(h, start)
        received(h, 2, 0, y_dev)
        received(h, 3, 1, y_dev)
        forward_y(h, start)

    def event_diagonal(h):
        received(h, 6, 0, d_blk)
        hop(h, 12, 0, d_blk, c_dev).start()
        received(h, 7, 1, d_blk)
        hop(h, 13, 1, d_blk, c_dev).start()

    def event_core(h):
        load(h, 0).wait()
        load(h, 1).wait()
        for slot in (4, 8, 10, 12):
            received(h, slot, 0, c_dev)
        for slot in (5, 9, 11, 13):
            received(h, slot, 1, c_dev)

    def o_cols(src_z, h):
        return o_ref.at[:, pl.ds(pl.multiple_of((src_z * HEADS + h) * HEAD_DIM, HEAD_DIM), HEAD_DIM)]

    def o_copy(h, target):
        return pltpu.make_async_remote_copy(
            src_ref=o_buf.at[h], dst_ref=o_cols(z, h), send_sem=o_send.at[h, target], recv_sem=o_recv.at[h, z],
            device_id=(target, cp), device_id_type=MESH)

    def o_forward(h):
        far = jnp.where(z == 1, 3, 0)
        target = jnp.where(z == 1, 0, 3)
        return pltpu.make_async_remote_copy(
            src_ref=o_cols(far, h), dst_ref=o_cols(far, h), send_sem=o_send.at[h, 4], recv_sem=o_recv.at[h, far],
            device_id=(target, cp), device_id_type=MESH)

    def o_received(h, src_z):
        pltpu.make_async_remote_copy(
            src_ref=o_buf.at[h], dst_ref=o_cols(src_z, h), send_sem=o_send.at[h, src_z], recv_sem=o_recv.at[h, src_z],
            device_id=(z, cp), device_id_type=MESH).wait_recv()

    sends_to = ((1, 2), (0, 2, 3), (3, 1, 0), (2, 1))

    def o_start(h):
        pltpu.make_async_copy(o_buf.at[h], o_cols(z, h), o_local.at[h]).start()
        for src in range(4):
            @pl.when(z == src)
            def _():
                for target in sends_to[src]:
                    o_copy(h, target).start()

    def o_pass(h):
        @pl.when((z == 1) | (z == 2))
        def _():
            o_received(h, jnp.where(z == 1, 3, 0))
            o_forward(h).start()

    key_iota = lax.broadcasted_iota(jnp.int32, (BLOCK, TILE_Q), 0)
    row_iota = lax.broadcasted_iota(jnp.int32, (BLOCK, TILE_Q), 1)

    def attend(h, t):
        q = q_ref[h, t * TILE_Q:(t + 1) * TILE_Q, :]

        def scores(j):
            return dot_rows(k_buf[h, j], q)

        def soft(s, j):
            m_old = m_s[...]
            m_new = jnp.maximum(m_old, jnp.max(s, axis=0, keepdims=True))
            alpha = jnp.exp2((m_old - m_new) * EXP_SCALE)
            p = jnp.exp2((s - m_new) * EXP_SCALE)
            l_s[...] = l_s[...] * alpha + jnp.sum(p, axis=0, keepdims=True)
            a_s[...] = a_s[...] * alpha + jnp.dot(v_buf[h, j], p.astype(BF16), preferred_element_type=F32)
            m_s[...] = m_new

        lo = jnp.maximum(cp - (WINDOW_BLOCKS - 1), 0) if windowed else 0
        count = cp - lo
        s0[...] = scores(cp)
        s1[...] = scores(jnp.minimum(lo, cp))
        s = jnp.where(key_iota <= row_iota + t * TILE_Q, s0[...], -1e30)
        m_new = jnp.max(s, axis=0, keepdims=True)
        p = jnp.exp2((s - m_new) * EXP_SCALE)
        l_s[...] = jnp.sum(p, axis=0, keepdims=True)
        a_s[...] = jnp.dot(v_buf[h, cp], p.astype(BF16), preferred_element_type=F32)
        m_s[...] = m_new

        def pair(i, _):
            j = lo + 2 * i
            s0[...] = scores(j + 1)
            soft(s1[...], j)
            s1[...] = scores(jnp.minimum(j + 2, cp))
            soft(s0[...], j + 1)
            return 0

        lax.fori_loop(0, count // 2, pair, 0)

        @pl.when(count % 2 == 1)
        def _():
            soft(s1[...], cp - 1)

        if windowed:
            @pl.when(cp >= WINDOW_BLOCKS)
            def _():
                s = scores(cp - WINDOW_BLOCKS)
                soft(jnp.where(key_iota > row_iota + t * TILE_Q, s, -1e30), cp - WINDOW_BLOCKS)

        o_buf[h, t * TILE_Q:(t + 1) * TILE_Q, :] = (a_s[...] / l_s[...]).T.astype(BF16)

    own(0, start)
    event_neighbours(0)
    own(1, start)
    own(2, start)
    event_diagonal(0)

    def head(h, _):
        event_core(h)
        attend(h, 0)

        @pl.when(h + 1 < HEADS)
        def _():
            event_neighbours(h + 1)

        @pl.when(h + 3 < HEADS)
        def _():
            own(h + 3, start)

        attend(h, 1)
        o_start(h)

        @pl.when(h + 1 < HEADS)
        def _():
            event_diagonal(h + 1)

        @pl.when(h >= 1)
        def _():
            o_pass(h - 1)
        return 0

    lax.fori_loop(0, HEADS, head, 0)
    o_pass(HEADS - 1)

    def drain(h, _):
        own(h, wait_send)
        forward_x(h, wait_send)
        forward_y(h, wait_send)
        hop(h, 12, 0, d_blk, c_dev).wait_send()
        hop(h, 13, 1, d_blk, c_dev).wait_send()
        pltpu.make_async_copy(o_buf.at[h], o_cols(z, h), o_local.at[h]).wait()
        for me in range(4):
            @pl.when(z == me)
            def _():
                for target in sends_to[me]:
                    o_copy(h, target).wait_send()
                for src in range(4):
                    if src != me and (me, src) not in ((1, 3), (2, 0)):
                        o_received(h, src)

        @pl.when((z == 1) | (z == 2))
        def _():
            o_forward(h).wait_send()
        return 0

    lax.fori_loop(0, HEADS, drain, 0)


def attention_call(layer, windowed, q, k, vt):
    return pl.pallas_call(
        functools.partial(attention_kernel, windowed),
        out_shape=jax.ShapeDtypeStruct((BLOCK, 4 * HEADS * HEAD_DIM), BF16),
        in_specs=[vmem(), hbm(), hbm()],
        out_specs=hbm(),
        scratch_shapes=[
            pltpu.VMEM((HEADS, 8, BLOCK, HEAD_DIM), BF16),
            pltpu.VMEM((HEADS, 8, HEAD_DIM, BLOCK), BF16),
            pltpu.VMEM((HEADS, BLOCK, HEAD_DIM), BF16),
            pltpu.VMEM((1, TILE_Q), F32),
            pltpu.VMEM((1, TILE_Q), F32),
            pltpu.VMEM((HEAD_DIM, TILE_Q), F32),
            pltpu.VMEM((BLOCK, TILE_Q), F32),
            pltpu.VMEM((BLOCK, TILE_Q), F32),
            pltpu.SemaphoreType.DMA((HEADS, 2)),
            pltpu.SemaphoreType.DMA((HEADS, 14)),
            pltpu.SemaphoreType.DMA((HEADS, 14)),
            pltpu.SemaphoreType.DMA((HEADS, 5)),
            pltpu.SemaphoreType.DMA((HEADS, 4)),
            pltpu.SemaphoreType.DMA((HEADS,)),
        ],
        compiler_params=pltpu.CompilerParams(
            vmem_limit_bytes=VMEM_LIMIT, collective_id=1 + layer, has_side_effects=True),
        cost_estimate=pl.CostEstimate(flops=50_000_000_000, bytes_accessed=40_000_000, transcendentals=0),
        name=f"attention{layer}",
    )(q, k, vt)


def mlp_kernel(layer, x_ref, gain_ref, wg_ref, wu_ref, wd_ref, out_ref,
               wg, wu, wd, xv, pv, rv, sv, load_sem, r_send, r_recv, s_send, s_recv, x_send, x_recv, x_local):
    z = lax.axis_index("tp")
    cp = lax.axis_index("cp")
    inner = (z == 1) | (z == 2)
    partner = z + 1 - 2 * (z % 2)
    middle = jnp.where(inner, 3 - z, z)
    per_chunk = CHUNK // PIECE
    pieces = BLOCK // PIECE

    loads = [
        pltpu.make_async_copy(x_ref, xv, load_sem.at[0]),
        pltpu.make_async_copy(wg_ref.at[layer], wg, load_sem.at[1]),
        pltpu.make_async_copy(wu_ref.at[layer], wu, load_sem.at[2]),
        pltpu.make_async_copy(wd_ref.at[layer], wd, load_sem.at[3]),
    ]
    for copy in loads:
        copy.start()

    barrier = pltpu.get_barrier_semaphore()
    pl.semaphore_signal(barrier, inc=1, device_id=(partner, cp), device_id_type=MESH)

    @pl.when(inner)
    def _():
        pl.semaphore_signal(barrier, inc=1, device_id=(3 - z, cp), device_id_type=MESH)
        pl.semaphore_wait(barrier, 2)

    @pl.when(jnp.logical_not(inner))
    def _():
        pl.semaphore_wait(barrier, 1)

    gain = gain_ref[layer:layer + 1, :].astype(F32)
    for copy in loads:
        copy.wait()

    def rows_of(i, size):
        return pl.ds(pl.multiple_of(i * size, size), size)

    def remote(src, dst, send, recv, i, dev):
        return pltpu.make_async_remote_copy(
            src_ref=src.at[rows_of(i, PIECE), :], dst_ref=dst.at[rows_of(i, PIECE), :],
            send_sem=send.at[i], recv_sem=recv.at[i], device_id=(dev, cp), device_id_type=MESH)

    def copy_r(i):
        return remote(pv, rv, r_send, r_recv, i, partner)

    def copy_s(i):
        return remote(pv, sv, s_send, s_recv, i, middle)

    def copy_x(i):
        return remote(xv, out_ref, x_send, x_recv, i, partner)

    def copy_local(i):
        return pltpu.make_async_copy(xv.at[rows_of(i, PIECE), :], out_ref.at[rows_of(i, PIECE), :], x_local.at[i])

    def compute(j):
        rows = rows_of(j, CHUNK)
        normed = normalize(xv[rows, :], gain)
        gate = jnp.dot(normed, wg[...], preferred_element_type=F32)
        up = jnp.dot(normed, wu[...], preferred_element_type=F32)
        act = (gate * jax.nn.sigmoid(gate) * up).astype(BF16)
        pv[rows, :] = jnp.dot(act, wd[...], preferred_element_type=F32).astype(BF16)

    def add_end(i):
        rows = rows_of(i, PIECE)
        copy_r(i).wait_recv()
        pv[rows, :] = (pv[rows, :].astype(F32) + rv[rows, :].astype(F32)).astype(BF16)
        copy_s(i).start()

    def add_middle(i):
        rows = rows_of(i, PIECE)
        copy_s(i).wait_recv()
        total = pv[rows, :].astype(F32) + sv[rows, :].astype(F32)
        xv[rows, :] = (xv[rows, :].astype(F32) + total).astype(BF16)
        copy_x(i).start()
        copy_local(i).start()

    def step(j, _):
        @pl.when(j < BLOCK // CHUNK)
        def _():
            compute(j)

            @pl.when(jnp.logical_not(inner))
            def _():
                for k in range(per_chunk):
                    copy_r(j * per_chunk + k).start()

        @pl.when(inner & (j >= 1))
        def _():
            def piece(k, _):
                i = (j - 1) * per_chunk + k
                add_end(i)

                @pl.when(i >= 1)
                def _():
                    add_middle(i - 1)
                return 0

            lax.fori_loop(0, per_chunk, piece, 0)
        return 0

    lax.fori_loop(0, BLOCK // CHUNK + 1, step, 0)

    @pl.when(inner)
    def _():
        add_middle(pieces - 1)

        def drain(i, _):
            copy_s(i).wait_send()
            copy_x(i).wait_send()
            copy_local(i).wait()
            return 0

        lax.fori_loop(0, pieces, drain, 0)

    @pl.when(jnp.logical_not(inner))
    def _():
        def drain(i, _):
            copy_r(i).wait_send()
            copy_x(i).wait_recv()
            return 0

        lax.fori_loop(0, pieces, drain, 0)


def mlp_call(layer, x, gain, wg, wu, wd):
    pieces = BLOCK // PIECE
    return pl.pallas_call(
        functools.partial(mlp_kernel, layer),
        out_shape=jax.ShapeDtypeStruct((BLOCK, WIDTH), BF16),
        in_specs=[hbm(), vmem(), hbm(), hbm(), hbm()],
        out_specs=hbm(),
        scratch_shapes=[
            pltpu.VMEM((WIDTH, FFN), BF16),
            pltpu.VMEM((WIDTH, FFN), BF16),
            pltpu.VMEM((FFN, WIDTH), BF16),
            pltpu.VMEM((BLOCK, WIDTH), BF16),
            pltpu.VMEM((BLOCK, WIDTH), BF16),
            pltpu.VMEM((BLOCK, WIDTH), BF16),
            pltpu.VMEM((BLOCK, WIDTH), BF16),
            pltpu.SemaphoreType.DMA((4,)),
        ] + [pltpu.SemaphoreType.DMA((pieces,))] * 7,
        compiler_params=pltpu.CompilerParams(
            vmem_limit_bytes=VMEM_LIMIT, collective_id=3 + layer, has_side_effects=True),
        cost_estimate=pl.CostEstimate(flops=100_000_000_000, bytes_accessed=40_000_000, transcendentals=0),
        name=f"mlp{layer}",
    )(x, gain, wg, wu, wd)


def solution(mesh):
    def local_step(x_in, positions, attn_gain, mlp_gain, w_query, b_query, w_key, b_key, w_value, b_value,
                   w_out, w_gate, w_up, w_down):
        cp = lax.axis_index("cp")
        rows = w_out.shape[1] // 8
        w_slice = lax.dynamic_slice_in_dim(w_out, cp * rows, rows, axis=1)
        w_full = [lax.all_gather(w_slice[l], ("tp", "cp"), axis=0, tiled=True) for l in range(2)]

        inv_freq = 1.0 / (1000000.0 ** (jnp.arange(0, HEAD_DIM, 2, dtype=F32) / HEAD_DIM))
        angles = positions.astype(F32)[:, None] * inv_freq[None, :]
        cos, sin = jnp.cos(angles), jnp.sin(angles)
        cos = jnp.concatenate([cos, cos], axis=1)
        sin = jnp.concatenate([-sin, sin], axis=1)

        hidden = x_in
        caches = []
        for layer in range(2):
            bias = jnp.stack([b_query[layer], b_key[layer], b_value[layer]])
            q, k, vt, k_out, v_out = qkv_call(layer, hidden, attn_gain, w_query, w_key, w_value, bias, cos, sin)
            heads = attention_call(layer, layer == 1, q, k, vt)
            hidden = (hidden.astype(F32) + jnp.dot(heads, w_full[layer], preferred_element_type=F32)).astype(BF16)
            hidden = mlp_call(layer, hidden, mlp_gain, w_gate, w_up, w_down)
            caches.append(k_out.reshape(BLOCK, HEADS, HEAD_DIM))
            caches.append(v_out.reshape(BLOCK, HEADS, HEAD_DIM))
        return hidden, caches[0], caches[1], caches[2], caches[3]

    weight_col = P(None, None, "tp")
    bias_col = P(None, "tp")
    weight_row = P(None, "tp", None)
    replicated = P(None, None)
    cache_spec = P("cp", "tp", None)
    in_specs = (P("cp", None), P("cp"), replicated, replicated, weight_col, bias_col, weight_col, bias_col,
                weight_col, bias_col, weight_row, weight_col, weight_col, weight_row)
    out_specs = (P("cp", None), cache_spec, cache_spec, cache_spec, cache_spec)
    return jax.shard_map(local_step, mesh=mesh, in_specs=in_specs, out_specs=out_specs, check_vma=False)
```

```python
import functools
import types

import jax
import jax.numpy as jnp
from jax import lax
from jax.experimental import pallas as pl
from jax.experimental.pallas import tpu as pltpu
from jax.sharding import PartitionSpec as P

MESH = pl.DeviceIdType.MESH
BF16 = jnp.bfloat16
F32 = jnp.float32
DMA = pltpu.SemaphoreType.DMA
HEAD_DIM = 128
HEADS = 5
BLOCK = 1024
BLOCKS = 8
COLUMN = 4
WIDTH = 2560
FFN = 1728
WINDOW_BLOCKS = 4
CHUNK = 128
SLICE = 16
ROWS = 256
PIECE = 32
SKEW = 2
TAIL = (32, 32, 16, 16, 16, 16)
TAIL_SKEW = 3
TILE_Q = 512
EXP_SCALE = HEAD_DIM ** -0.5 * 1.4426950408889634
MASKED = -1e30
VMEM_LIMIT = 67_043_328
FULL_SHAPE = (HEADS, COLUMN - 1, BLOCKS, SLICE, WIDTH)
PARAMS = functools.partial(pltpu.CompilerParams, vmem_limit_bytes=VMEM_LIMIT, has_side_effects=True)


def hbm():
    return pl.BlockSpec(memory_space=pl.ANY)


def vmem():
    return pl.BlockSpec(memory_space=pltpu.VMEM)


def bf16(*shape):
    return jax.ShapeDtypeStruct(shape, BF16)


def vmem_bf16(*shape):
    return pltpu.VMEM(shape, BF16)


def vmem_f32(*shape):
    return pltpu.VMEM(shape, F32)


def cost(flops):
    return pl.CostEstimate(flops=int(flops), bytes_accessed=int(5e7), transcendentals=0)


def loop(lo, hi):
    def wrap(body):
        def step(i, carry):
            body(i)
            return carry
        lax.fori_loop(lo, hi, step, 0)
    return wrap


def scoped(name):
    def wrap(fn):
        def inner(*args):
            with jax.named_scope(name):
                return fn(*args)
        return inner
    return wrap


def start(copy):
    copy.start()


def wait(copy):
    copy.wait()


def wait_send(copy):
    copy.wait_send()


def rows_of(i, size=ROWS):
    return pl.ds(pl.multiple_of(i * size, size), size)


def lanes_of(i):
    return rows_of(i, HEAD_DIM)


def dot_rows(a, b):
    return lax.dot_general(a, b, (((1,), (1,)), ((), ())), preferred_element_type=F32)


def normalize(rows, gain):
    rows_f = rows.astype(F32)
    variance = jnp.mean(rows_f * rows_f, axis=-1, keepdims=True)
    return (rows_f * lax.rsqrt(variance + 1e-6) * gain).astype(BF16)


def rotate(part, cos, sin):
    return (part * cos + pltpu.roll(part, HEAD_DIM // 2, 1) * sin).astype(BF16)


def remote(src, dst, send, recv, z, cp):
    return pltpu.make_async_remote_copy(
        src_ref=src, dst_ref=dst, send_sem=send, recv_sem=recv, device_id=(z, cp), device_id_type=MESH)


SENDS_TO = ((1, 2), (0, 2, 3), (3, 1, 0), (2, 1))


def is_middle(z):
    return (z == 1) | (z == 2)


def far_end(z):
    return jnp.where(z == 1, 3, 0)


def other_end(z):
    return jnp.where(z == 1, 0, 3)


def on_each(z, fn):
    for me in range(COLUMN):
        pl.when(z == me)(functools.partial(fn, me))


def plane(cp):
    x_dev = cp + 2 - 4 * ((cp // 2) % 2)
    y_dev = cp + 4 - 8 * (cp // 4)
    c_dev = cp + 1 - 2 * (cp % 2)
    d_dev = x_dev + 4 - 8 * (x_dev // 4)
    return x_dev, y_dev, c_dev, d_dev


def signal(z, cp):
    pl.semaphore_signal(pltpu.get_barrier_semaphore(), inc=1, device_id=(z, cp), device_id_type=MESH)


def arrive(count):
    pl.semaphore_wait(pltpu.get_barrier_semaphore(), count)


def greet_column(z, cp):
    for step in range(1, COLUMN):
        signal(lax.rem(z + step, COLUMN), cp)


def greet_plane(z, cp):
    for other in plane(cp)[:3]:
        signal(z, other)


class ColumnGather:
    def __init__(self, z, cp, part, landing, send, recv):
        self.z, self.cp, self.part, self.landing, self.send, self.recv = z, cp, part, landing, send, recv

    def copy(self, me, target):
        return remote(self.part(me, target), self.landing(me, target), self.send.at[target], self.recv.at[me], target, self.cp)

    def forward(self):
        far, target = far_end(self.z), other_end(self.z)
        return remote(self.landing(far, self.z), self.landing(far, target), self.send.at[COLUMN], self.recv.at[far],
                      target, self.cp)

    def received(self, src):
        ref = self.landing(src, self.z)
        remote(ref, ref, self.send.at[COLUMN], self.recv.at[src], self.z, self.cp).wait_recv()

    def each(self, action):
        def fn(me):
            for target in SENDS_TO[me]:
                action(self.copy(me, target))
        on_each(self.z, fn)

    def begin(self):
        self.each(start)

    def passing(self):
        @pl.when(is_middle(self.z))
        def _():
            self.received(far_end(self.z))
            self.forward().start()

    def finish(self):
        def fn(me):
            for src in range(COLUMN):
                if src != me and not (me in (1, 2) and abs(src - me) == 2):
                    self.received(src)
        on_each(self.z, fn)

    def drain(self):
        self.each(wait_send)

        @pl.when(is_middle(self.z))
        def _():
            self.forward().wait_send()


def column_sems(*lead):
    return [DMA((*lead, COLUMN + 1)), DMA((*lead, COLUMN))]


class PlaneExchange:
    OWN, FROM_X, FROM_Y, FROM_D, COPIES = range(6), range(6, 9), range(9, 12), range(12, 14), 14

    def __init__(self, z, cp, ref, send, recv, own_src=None):
        self.z, self.cp, self.ref, self.send, self.recv = z, cp, ref, send, recv
        self.own_src = own_src or (lambda item, part: ref(item, part, cp))
        x_dev, y_dev, c_dev, d_dev = plane(cp)
        self.routes = [(part, cp, dev) for dev in (x_dev, y_dev, c_dev) for part in range(2)]
        self.routes += [(0, x_dev, y_dev), (0, x_dev, c_dev), (1, x_dev, c_dev)]
        self.routes += [(1, y_dev, x_dev), (0, y_dev, c_dev), (1, y_dev, c_dev)]
        self.routes += [(0, d_dev, c_dev), (1, d_dev, c_dev)]

    def copy(self, item, slot):
        part, block, dev = self.routes[slot]
        dst = self.ref(item, part, block)
        src = self.own_src(item, part) if slot in self.OWN else dst
        return remote(src, dst, self.send.at[item, slot], self.recv.at[item, slot], self.z, dev)

    def group(self, item, slots, action=start):
        for slot in slots:
            action(self.copy(item, slot))

    def arrivals(self, item, slots, block):
        for slot in slots:
            ref = self.ref(item, self.routes[slot][0], block)
            remote(ref, ref, self.send.at[item, slot], self.recv.at[item, slot], self.z, plane(self.cp)[2]).wait_recv()

    def own(self, item, action=start):
        self.group(item, self.OWN, action)

    @scoped("near")
    def near(self, item):
        x_dev, y_dev, _, _ = plane(self.cp)
        self.arrivals(item, self.OWN[:2], x_dev)
        self.group(item, self.FROM_X)
        self.arrivals(item, self.OWN[2:4], y_dev)
        self.group(item, self.FROM_Y)

    @scoped("diagonal")
    def diagonal(self, item):
        d_dev = plane(self.cp)[3]
        for passed, slots in ((self.FROM_X, self.FROM_D[:1]), (self.FROM_Y, self.FROM_D[1:])):
            self.arrivals(item, passed[:1], d_dev)
            self.group(item, slots)

    @scoped("core")
    def core(self, item):
        x_dev, y_dev, c_dev, d_dev = plane(self.cp)
        for slots, block in ((self.OWN[4:], c_dev), (self.FROM_X[1:], self.mate(x_dev)),
                             (self.FROM_Y[1:], self.mate(y_dev)), (self.FROM_D, self.mate(d_dev))):
            self.arrivals(item, slots, block)

    @staticmethod
    def mate(dev):
        return plane(dev)[2]

    def drain(self, item, own=True):
        if own:
            self.own(item, wait_send)
        for slots in (self.FROM_X, self.FROM_Y, self.FROM_D):
            self.group(item, slots, wait_send)


def plane_sems(items):
    return [DMA((items, PlaneExchange.COPIES))] * 2


def weight_slices(layer, z, cp, src, full, send, recv):
    def landing(me, target):
        return full.at[:, lax.rem(me - target + COLUMN, COLUMN) - 1, cp]
    return ColumnGather(z, cp, lambda me, target: src.at[layer, :, cp], landing, send, recv)


def weight_exchange(group, z, cp, full, send, recv):
    half = SLICE // 2

    def ref(item, part, block):
        return full.at[pl.ds(item * group, group), :, block, part * half:(part + 1) * half]
    return PlaneExchange(z, cp, ref, send, recv)


ATTENTION_SCRATCH = [
    vmem_bf16(BLOCK, WIDTH),
    vmem_bf16(HEADS, BLOCK, HEAD_DIM),
    vmem_bf16(HEADS, BLOCK, COLUMN * HEAD_DIM),
    vmem_f32(BLOCK, WIDTH),
    vmem_bf16(2, COLUMN, BLOCKS, SLICE, WIDTH),
    vmem_f32(1, TILE_Q),
    vmem_f32(1, TILE_Q),
    vmem_f32(HEAD_DIM, TILE_Q),
    vmem_f32(BLOCK, TILE_Q),
    vmem_f32(BLOCK, TILE_Q),
    DMA((BLOCK // ROWS,)), DMA((2, COLUMN)), DMA((BLOCK // ROWS,)),
] + column_sems(HEADS, 2)
TILES = BLOCK // TILE_Q


def attention_parts(layer, windowed, z, cp, k_buf, v_buf, slot_of, x_ref, wo_ref, full_ref, out_ref,
                    xh, q_buf, o_all, acc, wo_buf, m_s, l_s, a_s, s0, s1, x_sem, wo_sem, out_sem, o_send, o_recv):
    def load_x(i):
        return pltpu.make_async_copy(x_ref.at[rows_of(i), :], xh.at[rows_of(i), :], x_sem.at[i])

    def gather(h, t):
        def part(me, target):
            return o_all.at[h, rows_of(t, TILE_Q), lanes_of(me)]
        return ColumnGather(z, cp, part, part, o_send.at[h, t], o_recv.at[h, t])

    def o_pass(h):
        for t in range(TILES):
            gather(h, t).passing()

    key_iota = lax.broadcasted_iota(jnp.int32, (BLOCK, TILE_Q), 0)
    row_iota = lax.broadcasted_iota(jnp.int32, (BLOCK, TILE_Q), 1)

    @scoped("attend")
    def attend(h, t):
        q = q_buf[h, rows_of(t, TILE_Q), :]
        ks, vs = k_buf.at[slot_of(h)], v_buf.at[slot_of(h)]

        def scores(j):
            return dot_rows(ks[j], q)

        def soft(s, j, first=False):
            m_new = jnp.max(s, axis=0, keepdims=True)
            if not first:
                m_old = m_s[...]
                m_new = jnp.maximum(m_old, m_new)
                alpha = jnp.exp2((m_old - m_new) * EXP_SCALE)
            p = jnp.exp2((s - m_new) * EXP_SCALE)
            norm = jnp.sum(p, axis=0, keepdims=True)
            out = jnp.dot(vs[j], p.astype(BF16), preferred_element_type=F32)
            l_s[...] = norm if first else l_s[...] * alpha + norm
            a_s[...] = out if first else a_s[...] * alpha + out
            m_s[...] = m_new

        lo = jnp.maximum(cp - (WINDOW_BLOCKS - 1), 0) if windowed else 0
        count = cp - lo
        s0[...] = scores(cp)
        s1[...] = scores(jnp.minimum(lo, cp))
        soft(jnp.where(key_iota <= row_iota + t * TILE_Q, s0[...], MASKED), cp, True)

        @loop(0, count // 2)
        def _(i):
            j = lo + 2 * i
            s0[...] = scores(j + 1)
            soft(s1[...], j)
            s1[...] = scores(jnp.minimum(j + 2, cp))
            soft(s0[...], j + 1)

        @pl.when(count % 2 == 1)
        def _():
            soft(s1[...], cp - 1)

        if windowed:
            @pl.when(cp >= WINDOW_BLOCKS)
            def _():
                edge = cp - WINDOW_BLOCKS
                soft(jnp.where(key_iota > row_iota + t * TILE_Q, scores(edge), MASKED), edge)

        o_all[h, rows_of(t, TILE_Q), lanes_of(z)] = (a_s[...] / l_s[...]).T.astype(BF16)

    def load_wo(h, action=start):
        slot = h % 2
        for part in range(COLUMN):
            rel = lax.rem(part - z + COLUMN, COLUMN)

            def load(src):
                action(pltpu.make_async_copy(src, wo_buf.at[slot, part], wo_sem.at[slot, part]))
            pl.when(rel == 0)(lambda: load(wo_ref.at[layer, h]))
            pl.when(rel > 0)(lambda: load(full_ref.at[h, rel - 1]))

    def store_out(i):
        return pltpu.make_async_copy(xh.at[rows_of(i), :], out_ref.at[rows_of(i), :], out_sem.at[i])

    @scoped("apply_wo")
    def apply_wo(h):
        for t in range(TILES):
            gather(h, t).finish()
        load_wo(h, wait)

        @loop(0, BLOCK // ROWS)
        def _(i):
            rows = rows_of(i)
            weight = wo_buf[h % 2].reshape(COLUMN * HEAD_DIM, WIDTH)
            part = jnp.dot(o_all[h, rows, :], weight, preferred_element_type=F32)

            @pl.when(h == 0)
            def _():
                acc[rows, :] = part

            @pl.when((h > 0) & (h < HEADS - 1))
            def _():
                acc[rows, :] += part

            @pl.when(h == HEADS - 1)
            def _():
                load_x(i).wait()
                xh[rows, :] = (xh[rows, :].astype(F32) + (acc[rows, :] + part)).astype(BF16)
                store_out(i).start()

    def start_x():
        for i in range(BLOCK // ROWS):
            load_x(i).start()

    def drain(h):
        for t in range(TILES):
            gather(h, t).drain()

    def settle():
        for i in range(BLOCK // ROWS):
            store_out(i).wait()

    return types.SimpleNamespace(
        load_x=load_x, start_x=start_x, attend=attend, o_start=lambda h, t: gather(h, t).begin(), o_pass=scoped("o_pass")(o_pass),
        load_wo=load_wo, apply_wo=apply_wo, drain=drain, settle=settle)


def first_kernel(x_ref, gain_ref, wq_ref, wk_ref, wv_ref, bias_ref, cos_ref, sin_ref, wo_ref,
                 out_ref, k_out, v_out, full_ref, next_ref,
                 w_buf, k_buf, v_buf, v_nat, w_sem, kv_sem, send_sem, recv_sem, *rest):
    z = lax.axis_index("tp")
    cp = lax.axis_index("cp")
    count = len(ATTENTION_SCRATCH)
    xh, q_buf = rest[:2]
    z_send, z_recv, n_send, n_recv, p_send, p_recv = rest[count:]
    slices = weight_slices(0, z, cp, wo_ref, full_ref, z_send, z_recv)
    next_slices = weight_slices(1, z, cp, wo_ref, next_ref, n_send, n_recv)
    weights = weight_exchange(1, z, cp, full_ref, p_send, p_recv)
    kv = PlaneExchange(z, cp, lambda h, part, block: (k_buf, v_buf)[part].at[h, block], send_sem, recv_sem)
    parts = attention_parts(0, False, z, cp, k_buf, v_buf, lambda h: h, x_ref, wo_ref, full_ref, out_ref, *rest[:count])

    def load_w(h, action):
        slot = h % 2
        for i, w in enumerate((wq_ref, wk_ref, wv_ref)):
            action(pltpu.make_async_copy(w.at[0, :, lanes_of(h)], w_buf.at[slot, :, lanes_of(i)], w_sem.at[slot, i]))

    greet_plane(z, cp)
    greet_column(z, cp)
    parts.start_x()
    load_w(0, start)
    arrive(6)
    slices.begin()
    next_slices.begin()
    gain = gain_ref[:1, :].astype(F32)

    @loop(0, BLOCK // ROWS)
    def _(i):
        parts.load_x(i).wait()
        xh[rows_of(i), :] = normalize(xh[rows_of(i), :], gain)

    def caches(h, action):
        action(pltpu.make_async_copy(k_buf.at[h, cp], k_out.at[h], kv_sem.at[h, 0]))
        action(pltpu.make_async_copy(v_nat.at[h], v_out.at[h], kv_sem.at[h, 1]))

    @loop(0, HEADS)
    @scoped("project")
    def _(h):
        @pl.when(h + 1 < HEADS)
        def _():
            load_w(h + 1, start)
        load_w(h, wait)

        @loop(0, BLOCK // ROWS)
        def _(i):
            rows = rows_of(i)
            proj = jnp.dot(xh[rows, :], w_buf[h % 2], preferred_element_type=F32)
            q, k, v = (proj[:, n * HEAD_DIM:(n + 1) * HEAD_DIM] + bias_ref[h, n:n + 1, :].astype(F32) for n in range(3))
            cos = cos_ref[rows, :]
            sin = sin_ref[rows, :]
            q_buf[h, rows, :] = rotate(q, cos, sin)
            k_buf[h, cp, rows, :] = rotate(k, cos, sin)
            v_nat[h, rows, :] = v.astype(BF16)
            v_buf[h, cp, :, rows] = v.T.astype(BF16)

        @pl.when(h == 0)
        def _():
            kv.own(0)

        @pl.when(h == 3)
        def _():
            kv.near(0)
            kv.own(1)
            kv.own(2)
        caches(h, start)

    slices.passing()
    kv.diagonal(0)
    parts.start_x()

    def between(h):
        @pl.when(h + 1 < HEADS)
        def _():
            kv.near(h + 1)

        @pl.when(h + 3 < HEADS)
        def _():
            kv.own(h + 3)

        @pl.when(h == HEADS - 2)
        def _():
            slices.finish()
            weights.own(0)
            weights.own(1)

        @pl.when(h == HEADS - 1)
        def _():
            weights.near(0)
            weights.own(2)

    def behind(h):
        pl.when(h == 0)(next_slices.passing)
        pl.when(h + 1 < HEADS)(lambda: kv.diagonal(h + 1))
        pl.when(h >= 1)(lambda: parts.o_pass(h - 1))

    @loop(0, HEADS * TILES)
    def _(i):
        h, t = i // TILES, i % TILES
        pl.when(t == 0)(lambda: kv.core(h))
        parts.attend(h, t)
        parts.o_start(h, t)
        pl.when(t == 0)(lambda: between(h))
        pl.when(t == TILES - 1)(lambda: behind(h))

    weights.near(1)
    weights.own(3)

    @loop(0, HEADS)
    def _(h):
        weights.diagonal(h)
        weights.core(h)
        parts.load_wo(h)

        @pl.when(h + 2 < HEADS)
        def _():
            weights.near(h + 2)

        @pl.when(h == 0)
        def _():
            weights.own(4)

        @pl.when(h == 2)
        def _():
            parts.o_pass(HEADS - 1)
        parts.apply_wo(h)

    @loop(0, HEADS)
    def _(h):
        kv.drain(h)
        weights.drain(h)
        caches(h, wait)
        parts.drain(h)

    next_slices.finish()
    next_slices.drain()
    slices.drain()
    parts.settle()


def first_call(*args):
    return pl.pallas_call(
        first_kernel,
        out_shape=(bf16(BLOCK, WIDTH), bf16(HEADS, BLOCK, HEAD_DIM), bf16(HEADS, BLOCK, HEAD_DIM),
                   bf16(*FULL_SHAPE), bf16(*FULL_SHAPE)),
        in_specs=[hbm(), vmem(), hbm(), hbm(), hbm(), vmem(), vmem(), vmem(), hbm()],
        out_specs=(hbm(),) * 5,
        scratch_shapes=[
            vmem_bf16(2, WIDTH, 3 * HEAD_DIM),
            vmem_bf16(HEADS, BLOCKS, BLOCK, HEAD_DIM),
            vmem_bf16(HEADS, BLOCKS, HEAD_DIM, BLOCK),
            vmem_bf16(HEADS, BLOCK, HEAD_DIM),
            DMA((2, 3)), DMA((HEADS, 2)),
        ] + plane_sems(HEADS) + ATTENTION_SCRATCH + column_sems() + column_sems() + plane_sems(HEADS),
        compiler_params=PARAMS(collective_id=1),
        cost_estimate=cost(7e10),
        name="front0",
    )(*args)


def second_kernel(x_ref, q_ref, k_ref, v_ref, wo_ref, full_ref, out_ref, k_buf, v_buf, q_sem, kv_sem, *rest):
    z = lax.axis_index("tp")
    cp = lax.axis_index("cp")
    parts = attention_parts(
        1, True, z, cp, k_buf, v_buf, lambda h: h % 2, x_ref, wo_ref, full_ref, out_ref, *rest)

    def load_kv(h, action):
        slot = h % 2
        for i, (src, dst) in enumerate(((k_ref, k_buf), (v_ref, v_buf))):
            action(pltpu.make_async_copy(src.at[h], dst.at[slot], kv_sem.at[slot, i]))

    greet_column(z, cp)
    load_q = pltpu.make_async_copy(q_ref, rest[1], q_sem)
    load_q.start()
    load_kv(0, start)
    load_q.wait()
    lag = 2

    def ahead(h):
        load_kv(h, wait)
        pl.when(h + 1 < HEADS)(lambda: load_kv(h + 1, start))

    def behind(h):
        pl.when(h >= 1)(lambda: parts.o_pass(h - 1))

        @pl.when(h >= lag)
        def _():
            parts.load_wo(h - lag + 1)
            parts.apply_wo(h - lag)

    @loop(0, HEADS * TILES)
    def _(i):
        h, t = i // TILES, i % TILES
        pl.when(t == 0)(lambda: ahead(h))
        parts.attend(h, t)

        @pl.when(i == 0)
        def _():
            arrive(3)
            parts.load_wo(0)
            parts.start_x()
        parts.o_start(h, t)
        pl.when(t == TILES - 1)(lambda: behind(h))

    parts.o_pass(HEADS - 1)

    @loop(HEADS - lag, HEADS)
    def _(h):
        @pl.when(h + 1 < HEADS)
        def _():
            parts.load_wo(h + 1)
        parts.apply_wo(h)

    @loop(0, HEADS)
    def _(h):
        parts.drain(h)
    parts.settle()


def second_call(*args):
    return pl.pallas_call(
        second_kernel,
        out_shape=bf16(BLOCK, WIDTH),
        in_specs=[hbm()] * 6,
        out_specs=hbm(),
        scratch_shapes=[
            vmem_bf16(2, BLOCKS, BLOCK, HEAD_DIM),
            vmem_bf16(2, BLOCKS, HEAD_DIM, BLOCK),
            DMA, DMA((2, 2)),
        ] + ATTENTION_SCRATCH,
        compiler_params=PARAMS(collective_id=2),
        cost_estimate=cost(5e10),
        name="front1",
    )(*args)


CHUNKS = BLOCK // CHUNK
PER_CHUNK = CHUNK // PIECE
REGULAR = (CHUNKS - 1) * PER_CHUNK


def mlp_kernel(layer, *refs):
    following = layer == 0
    x_ref, gain_ref, wg_ref, wu_ref, wd_ref, *refs = refs
    if following:
        next_gain, wq_ref, wk_ref, wv_ref, bias_ref, cos_ref, sin_ref, _, *refs = refs
        out_ref, q_out, k_out, v_out, k_all, v_all, full_ref, *refs = refs
    else:
        out_ref, *refs = refs
    wg, wu, wd, xv, pv, rv, sv, act, load_sem, r_send, r_recv, s_send, s_recv, x_send, x_recv, x_local, *refs = refs
    z = lax.axis_index("tp")
    cp = lax.axis_index("cp")
    inner = is_middle(z)
    outer = jnp.logical_not(inner)
    partner = z + 1 - 2 * (z % 2)
    middle = jnp.where(inner, 3 - z, z)
    tail = [(BLOCK - CHUNK + sum(TAIL[:i]), size, REGULAR + i) for i, size in enumerate(TAIL)]

    load_x, load_g, load_u, load_d = (
        pltpu.make_async_copy(src, dst, load_sem.at[i]) for i, (src, dst) in enumerate((
            (x_ref, xv), (wg_ref.at[layer], wg), (wu_ref.at[layer], wu), (wd_ref.at[layer], wd))))
    load_x.start()
    load_g.start()

    signal(partner, cp)
    pl.when(inner)(lambda: signal(middle, cp))
    if following:
        w_buf, q_st, k_st, v_st, n_st, w_sem, st_sem, send_sem, recv_sem, p_send, p_recv = refs
        greet_plane(z, cp)
        weights = weight_exchange(HEADS, z, cp, full_ref, p_send, p_recv)
    pl.when(inner)(lambda: arrive(5 if following else 2))
    pl.when(outer)(lambda: arrive(4 if following else 1))

    gain = gain_ref[layer:layer + 1, :].astype(F32)
    load_x.wait()

    def chunk_rows(j):
        return rows_of(j, CHUNK)

    def piece(i):
        return pl.multiple_of(i * PIECE, PIECE), PIECE, i

    def piece_copy(src, dst, send, recv, part, dev):
        at, size, i = part
        return remote(src.at[pl.ds(at, size), :], dst.at[pl.ds(at, size), :], send.at[i], recv.at[i], dev, cp)

    def copy_r(part):
        return piece_copy(pv, rv, r_send, r_recv, part, partner)

    def copy_s(part):
        return piece_copy(pv, sv, s_send, s_recv, part, middle)

    def copy_x(part):
        return piece_copy(xv, xv if following else out_ref, x_send, x_recv, part, partner)

    def copy_local(part):
        at, size, i = part
        return pltpu.make_async_copy(xv.at[pl.ds(at, size), :], out_ref.at[pl.ds(at, size), :], x_local.at[i])

    @scoped("activate")
    def activate(j):
        normed = normalize(xv[chunk_rows(j), :], gain)

        @pl.when(j == 0)
        def _():
            load_g.wait()
            load_u.start()
            load_d.start()
        gate = dot_rows(normed, wg[...])
        pl.when(j == 0)(load_u.wait)
        up = dot_rows(normed, wu[...])
        act[...] = (gate * jax.nn.sigmoid(gate) * up).astype(BF16)

    @scoped("down")
    def down(j):
        pl.when(j == 0)(load_d.wait)
        pv[chunk_rows(j), :] = jnp.dot(act[...], wd[...], preferred_element_type=F32).astype(BF16)

    @scoped("add_end")
    def add_end(part):
        rows = pl.ds(part[0], part[1])
        copy_r(part).wait_recv()
        pv[rows, :] = (pv[rows, :].astype(F32) + rv[rows, :].astype(F32)).astype(BF16)
        copy_s(part).start()

    @scoped("add_middle")
    def add_middle(part):
        rows = pl.ds(part[0], part[1])
        copy_s(part).wait_recv()
        total = pv[rows, :].astype(F32) + sv[rows, :].astype(F32)
        xv[rows, :] = (xv[rows, :].astype(F32) + total).astype(BF16)
        copy_x(part).start()
        copy_local(part).start()

    if following:
        load_w = [
            pltpu.make_async_copy(w.at[layer + 1], w_buf.at[i], w_sem.at[i])
            for i, w in enumerate((wq_ref, wk_ref, wv_ref))]
        gain_n = next_gain[layer + 1:layer + 2, :].astype(F32)

        def kv_ref(c, part, block):
            rows = chunk_rows(c)
            return v_all.at[:, block, :, rows] if part else k_all.at[:, block, rows, :]
        kv = PlaneExchange(z, cp, kv_ref, send_sem, recv_sem, lambda c, part: (k_st, v_st)[part].at[c % 2])

        def stores(c, action):
            rows = chunk_rows(c)
            slot = c % 2
            for i, (src, dst) in enumerate((
                    (q_st, q_out.at[:, rows, :]), (k_st, k_out.at[:, rows, :]), (n_st, v_out.at[:, rows, :]),
                    (k_st, kv_ref(c, 0, cp)), (v_st, kv_ref(c, 1, cp)))):
                action(pltpu.make_async_copy(src.at[slot], dst, st_sem.at[slot, i]))

        @scoped("x_wait")
        def x_wait(c):
            def land(parts):
                for part in parts:
                    copy_x(part).wait_recv()
                    copy_local(part).start()
            pl.when(outer & (c < CHUNKS - 1))(lambda: land([piece(c * PER_CHUNK + k) for k in range(PER_CHUNK)]))
            pl.when(outer & (c == CHUNKS - 1))(lambda: land(tail))

        def project(c):
            x_wait(c)
            pl.when(c >= 1)(lambda: kv.near(c - 1))

            @pl.when(c >= 2)
            def _():
                kv.diagonal(c - 2)
                kv.own(c - 2, wait_send)
                stores(c - 2, wait)

            with jax.named_scope("project"):
                rows = chunk_rows(c)
                slot = c % 2
                normed = normalize(xv[rows, :], gain_n)
                cos = cos_ref[rows, :]
                sin = sin_ref[rows, :]
                for which in range(3):
                    proj = jnp.dot(normed, w_buf[which], preferred_element_type=F32)
                    for h in range(HEADS):
                        part = proj[:, h * HEAD_DIM:(h + 1) * HEAD_DIM] + bias_ref[h, which:which + 1, :].astype(F32)
                        if which < 2:
                            (q_st, k_st)[which][slot, h] = rotate(part, cos, sin)
                        else:
                            n_st[slot, h] = part.astype(BF16)
                            v_st[slot, h] = part.T.astype(BF16)
            kv.own(c)
            stores(c, start)

    def serve(j, half):
        @loop(0, PER_CHUNK // 2)
        def _(k):
            i = j * PER_CHUNK + half * (PER_CHUNK // 2) + k
            add_end(piece(i))
            pl.when(i >= SKEW)(lambda: add_middle(piece(i - SKEW)))

    def serve_tail(first, last):
        for i in range(first, last):
            if i < len(tail):
                add_end(tail[i])
            if i == 0:
                for k in range(SKEW, 0, -1):
                    add_middle(piece(REGULAR - k))
            elif i >= TAIL_SKEW:
                add_middle(tail[i - TAIL_SKEW])

    tail_end = len(tail) + TAIL_SKEW
    lag = jnp.where(inner, 2, 5)

    @loop(0, CHUNKS)
    def _(j):
        activate(j)
        pl.when(inner & (j >= 1))(lambda: serve(j - 1, 0))
        down(j)

        @pl.when(outer & (j < CHUNKS - 1))
        def _():
            for k in range(PER_CHUNK):
                copy_r(piece(j * PER_CHUNK + k)).start()

        @pl.when(outer & (j == CHUNKS - 1))
        def _():
            for part in tail:
                copy_r(part).start()

        if following:
            @pl.when(j == 0)
            def _():
                weights.own(0)
                for copy in load_w:
                    copy.start()

            @pl.when(j == 1)
            def _():
                for copy in load_w:
                    copy.wait()
            pl.when(j == jnp.where(inner, 2, 3))(lambda: weights.near(0))
            pl.when(j == 5)(lambda: weights.diagonal(0))
            pl.when(j == 6)(lambda: weights.core(0))
            pl.when(j >= lag)(lambda: project(j - lag))
        pl.when(inner & (j >= 1))(lambda: serve(j - 1, 1))

    if following:
        @loop(CHUNKS - lag, CHUNKS)
        def _(c):
            pl.when(inner & (c == CHUNKS - 2))(lambda: serve_tail(0, 1))
            pl.when(inner & (c == CHUNKS - 1))(lambda: serve_tail(1, tail_end))
            project(c)
        kv.near(CHUNKS - 1)
        kv.diagonal(CHUNKS - 2)
        kv.diagonal(CHUNKS - 1)

        @loop(0, CHUNKS)
        def _(c):
            kv.core(c)
            kv.drain(c, False)

            @pl.when(c >= CHUNKS - 2)
            def _():
                kv.own(c, wait_send)
                stores(c, wait)
        weights.drain(0)
    else:
        pl.when(inner)(lambda: serve_tail(0, tail_end))

    def drain(part):
        @pl.when(inner)
        def _():
            copy_s(part).wait_send()
            copy_x(part).wait_send()
            copy_local(part).wait()

        @pl.when(outer)
        def _():
            copy_r(part).wait_send()
            if following:
                copy_local(part).wait()
            else:
                copy_x(part).wait_recv()

    @loop(0, REGULAR)
    def _(i):
        drain(piece(i))
    for part in tail:
        drain(part)


def mlp_call(layer, *args):
    outs = [bf16(BLOCK, WIDTH)]
    in_specs = [hbm(), vmem(), hbm(), hbm(), hbm()]
    scratch = [vmem_bf16(FFN, WIDTH)] * 3 + [vmem_bf16(BLOCK, WIDTH)] * 4 + [vmem_bf16(CHUNK, FFN), DMA((COLUMN,))]
    scratch += [DMA((REGULAR + len(TAIL),))] * 7
    aliases = {}
    if layer == 0:
        outs += [bf16(HEADS, BLOCK, HEAD_DIM)] * 3
        outs += [bf16(HEADS, BLOCKS, BLOCK, HEAD_DIM), bf16(HEADS, BLOCKS, HEAD_DIM, BLOCK), bf16(*FULL_SHAPE)]
        in_specs += [vmem(), hbm(), hbm(), hbm(), vmem(), vmem(), vmem(), hbm()]
        aliases = {len(in_specs) - 1: len(outs) - 1}
        scratch += [vmem_bf16(3, WIDTH, HEADS * HEAD_DIM)] + [vmem_bf16(2, HEADS, CHUNK, HEAD_DIM)] * 4
        scratch += [DMA((3,)), DMA((2, 5))] + plane_sems(CHUNKS) + plane_sems(1)
    return pl.pallas_call(
        functools.partial(mlp_kernel, layer),
        out_shape=tuple(outs),
        in_specs=in_specs,
        out_specs=(hbm(),) * len(outs),
        scratch_shapes=scratch,
        input_output_aliases=aliases,
        compiler_params=PARAMS(collective_id=3 + layer),
        cost_estimate=cost(1e11),
        name=f"mlp{layer}",
    )(*args)


def solution(mesh):
    def local_step(x_in, positions, attn_gain, mlp_gain, w_query, b_query, w_key, b_key, w_value, b_value,
                   w_out, w_gate, w_up, w_down):
        inv_freq = 1.0 / (1000000.0 ** (jnp.arange(0, HEAD_DIM, 2, dtype=F32) / HEAD_DIM))
        angles = positions.astype(F32)[:, None] * inv_freq[None, :]
        cos, sin = jnp.cos(angles), jnp.sin(angles)
        cos = jnp.concatenate([cos, cos], axis=1)
        sin = jnp.concatenate([-sin, sin], axis=1)

        w_gate = jnp.swapaxes(w_gate, 1, 2)
        w_up = jnp.swapaxes(w_up, 1, 2)
        wo = w_out.reshape(2, HEADS, BLOCKS, SLICE, WIDTH)
        bias = [jnp.stack([b.reshape(2, HEADS, HEAD_DIM)[layer] for b in (b_query, b_key, b_value)], axis=1)
                for layer in range(2)]
        hidden, k0, v0, _, full1 = first_call(x_in, attn_gain, w_query, w_key, w_value, bias[0], cos, sin, wo)
        hidden, q, k1, v1, k_all, v_all, full1 = mlp_call(
            0, hidden, mlp_gain, w_gate, w_up, w_down, attn_gain, w_query, w_key, w_value, bias[1], cos, sin, full1)
        hidden = second_call(hidden, q, k_all, v_all, wo, full1)
        hidden, = mlp_call(1, hidden, mlp_gain, w_gate, w_up, w_down)
        return (hidden,) + tuple(jnp.swapaxes(cache, 0, 1) for cache in (k0, v0, k1, v1))

    weight_col = P(None, None, "tp")
    bias_col = P(None, "tp")
    weight_row = P(None, "tp", None)
    replicated = P(None, None)
    cache_spec = P("cp", "tp", None)
    in_specs = (P("cp", None), P("cp"), replicated, replicated, weight_col, bias_col, weight_col, bias_col,
                weight_col, bias_col, weight_row, weight_col, weight_col, weight_row)
    out_specs = (P("cp", None), cache_spec, cache_spec, cache_spec, cache_spec)
    return jax.shard_map(local_step, mesh=mesh, in_specs=in_specs, out_specs=out_specs, check_vma=False)
```

```python
import functools
import types

import jax
import jax.numpy as jnp
from jax import lax
from jax.experimental import pallas as pl
from jax.experimental.pallas import tpu as pltpu
from jax.sharding import PartitionSpec as P

MESH = pl.DeviceIdType.MESH
BF16 = jnp.bfloat16
F32 = jnp.float32
DMA = pltpu.SemaphoreType.DMA
HEAD_DIM = 128
HEADS = 5
BLOCK = 1024
BLOCKS = 8
COLUMN = 4
WIDTH = 2560
FFN = 1728
WINDOW_BLOCKS = 4
CHUNK = 128
SLICE = 16
ROWS = 256
PIECE = 32
SKEW = 2
HEAD = (16, 16, 16, 16, 32, 32)
TAIL = (32, 32, 16, 16, 16, 16)
TAIL_SKEW = 3
TILE_Q = 512
EXP_SCALE = HEAD_DIM ** -0.5 * 1.4426950408889634
MASKED = -1e30
VMEM_LIMIT = 67_043_328
FFN_PARTS = (slice(0, 768), slice(768, FFN))
FULL_SHAPE = (HEADS, COLUMN - 1, BLOCKS, SLICE, WIDTH)
PARAMS = functools.partial(pltpu.CompilerParams, vmem_limit_bytes=VMEM_LIMIT, has_side_effects=True)


def hbm():
    return pl.BlockSpec(memory_space=pl.ANY)


def vmem():
    return pl.BlockSpec(memory_space=pltpu.VMEM)


def bf16(*shape):
    return jax.ShapeDtypeStruct(shape, BF16)


def vmem_bf16(*shape):
    return pltpu.VMEM(shape, BF16)


def vmem_f32(*shape):
    return pltpu.VMEM(shape, F32)


def cost(flops):
    return pl.CostEstimate(flops=int(flops), bytes_accessed=int(5e7), transcendentals=0)


def loop(lo, hi):
    def wrap(body):
        def step(i, carry):
            body(i)
            return carry
        lax.fori_loop(lo, hi, step, 0)
    return wrap


def scoped(name):
    def wrap(fn):
        def inner(*args):
            with jax.named_scope(name):
                return fn(*args)
        return inner
    return wrap


def start(copy):
    copy.start()


def wait(copy):
    copy.wait()


def wait_send(copy):
    copy.wait_send()


def rows_of(i, size=ROWS):
    return pl.ds(pl.multiple_of(i * size, size), size)


def lanes_of(i):
    return rows_of(i, HEAD_DIM)


def dot_rows(a, b):
    return lax.dot_general(a, b, (((1,), (1,)), ((), ())), preferred_element_type=F32)


def normalize(rows, gain):
    rows_f = rows.astype(F32)
    variance = jnp.mean(rows_f * rows_f, axis=-1, keepdims=True)
    return (rows_f * lax.rsqrt(variance + 1e-6) * gain).astype(BF16)


def rotate(part, cos, sin):
    return (part * cos + pltpu.roll(part, HEAD_DIM // 2, 1) * sin).astype(BF16)


def remote(src, dst, send, recv, z, cp):
    return pltpu.make_async_remote_copy(
        src_ref=src, dst_ref=dst, send_sem=send, recv_sem=recv, device_id=(z, cp), device_id_type=MESH)


SENDS_TO = ((1, 2), (0, 2, 3), (3, 1, 0), (2, 1))


def is_middle(z):
    return (z == 1) | (z == 2)


def far_end(z):
    return jnp.where(z == 1, 3, 0)


def other_end(z):
    return jnp.where(z == 1, 0, 3)


def on_each(z, fn):
    for me in range(COLUMN):
        pl.when(z == me)(functools.partial(fn, me))


def plane(cp):
    x_dev = cp + 2 - 4 * ((cp // 2) % 2)
    y_dev = cp + 4 - 8 * (cp // 4)
    c_dev = cp + 1 - 2 * (cp % 2)
    d_dev = x_dev + 4 - 8 * (x_dev // 4)
    return x_dev, y_dev, c_dev, d_dev


def signal(z, cp):
    pl.semaphore_signal(pltpu.get_barrier_semaphore(), inc=1, device_id=(z, cp), device_id_type=MESH)


def arrive(count):
    pl.semaphore_wait(pltpu.get_barrier_semaphore(), count)


def greet_column(z, cp):
    for step in range(1, COLUMN):
        signal(lax.rem(z + step, COLUMN), cp)


def greet_plane(z, cp):
    for other in plane(cp)[:3]:
        signal(z, other)


class ColumnGather:
    def __init__(self, z, cp, part, landing, send, recv):
        self.z, self.cp, self.part, self.landing, self.send, self.recv = z, cp, part, landing, send, recv

    def copy(self, me, target):
        return remote(self.part(me, target), self.landing(me, target), self.send.at[target], self.recv.at[me], target, self.cp)

    def forward(self):
        far, target = far_end(self.z), other_end(self.z)
        return remote(self.landing(far, self.z), self.landing(far, target), self.send.at[COLUMN], self.recv.at[far],
                      target, self.cp)

    def received(self, src):
        ref = self.landing(src, self.z)
        remote(ref, ref, self.send.at[COLUMN], self.recv.at[src], self.z, self.cp).wait_recv()

    def each(self, action):
        def fn(me):
            for target in SENDS_TO[me]:
                action(self.copy(me, target))
        on_each(self.z, fn)

    def begin(self):
        self.each(start)

    def passing(self):
        @pl.when(is_middle(self.z))
        def _():
            self.received(far_end(self.z))
            self.forward().start()

    def finish(self):
        def fn(me):
            for src in range(COLUMN):
                if src != me and not (me in (1, 2) and abs(src - me) == 2):
                    self.received(src)
        on_each(self.z, fn)

    def drain(self):
        self.each(wait_send)

        @pl.when(is_middle(self.z))
        def _():
            self.forward().wait_send()


def column_sems(*lead):
    return [DMA((*lead, COLUMN + 1)), DMA((*lead, COLUMN))]


class PlaneExchange:
    OWN, FROM_X, FROM_Y, FROM_D, COPIES = range(6), range(6, 9), range(9, 12), range(12, 14), 14

    def __init__(self, z, cp, ref, send, recv, own_src=None):
        self.z, self.cp, self.ref, self.send, self.recv = z, cp, ref, send, recv
        self.own_src = own_src or (lambda item, part: ref(item, part, cp))
        x_dev, y_dev, c_dev, d_dev = plane(cp)
        self.routes = [(part, cp, dev) for dev in (x_dev, y_dev, c_dev) for part in range(2)]
        self.routes += [(0, x_dev, y_dev), (0, x_dev, c_dev), (1, x_dev, c_dev)]
        self.routes += [(1, y_dev, x_dev), (0, y_dev, c_dev), (1, y_dev, c_dev)]
        self.routes += [(0, d_dev, c_dev), (1, d_dev, c_dev)]

    def copy(self, item, slot):
        part, block, dev = self.routes[slot]
        dst = self.ref(item, part, block)
        src = self.own_src(item, part) if slot in self.OWN else dst
        return remote(src, dst, self.send.at[item, slot], self.recv.at[item, slot], self.z, dev)

    def group(self, item, slots, action=start):
        for slot in slots:
            action(self.copy(item, slot))

    def arrivals(self, item, slots, block):
        for slot in slots:
            ref = self.ref(item, self.routes[slot][0], block)
            remote(ref, ref, self.send.at[item, slot], self.recv.at[item, slot], self.z, plane(self.cp)[2]).wait_recv()

    def own(self, item, action=start):
        self.group(item, self.OWN, action)

    @scoped("near")
    def near(self, item):
        x_dev, y_dev, _, _ = plane(self.cp)
        self.arrivals(item, self.OWN[:2], x_dev)
        self.group(item, self.FROM_X)
        self.arrivals(item, self.OWN[2:4], y_dev)
        self.group(item, self.FROM_Y)

    @scoped("diagonal")
    def diagonal(self, item):
        d_dev = plane(self.cp)[3]
        for passed, slots in ((self.FROM_X, self.FROM_D[:1]), (self.FROM_Y, self.FROM_D[1:])):
            self.arrivals(item, passed[:1], d_dev)
            self.group(item, slots)

    @scoped("core")
    def core(self, item):
        x_dev, y_dev, c_dev, d_dev = plane(self.cp)
        for slots, block in ((self.OWN[4:], c_dev), (self.FROM_X[1:], self.mate(x_dev)),
                             (self.FROM_Y[1:], self.mate(y_dev)), (self.FROM_D, self.mate(d_dev))):
            self.arrivals(item, slots, block)

    @staticmethod
    def mate(dev):
        return plane(dev)[2]

    def drain(self, item, own=True):
        if own:
            self.own(item, wait_send)
        for slots in (self.FROM_X, self.FROM_Y, self.FROM_D):
            self.group(item, slots, wait_send)


def plane_sems(items):
    return [DMA((items, PlaneExchange.COPIES))] * 2


def weight_slices(layer, z, cp, src, full, send, recv):
    def landing(me, target):
        return full.at[:, lax.rem(me - target + COLUMN, COLUMN) - 1, cp]
    return ColumnGather(z, cp, lambda me, target: src.at[layer, :, cp], landing, send, recv)


def weight_exchange(group, z, cp, full, send, recv):
    half = SLICE // 2

    def ref(item, part, block):
        return full.at[pl.ds(item * group, group), :, block, part * half:(part + 1) * half]
    return PlaneExchange(z, cp, ref, send, recv)


TILES = BLOCK // TILE_Q
COLS = WIDTH // TILE_Q
ATTENTION_SCRATCH = [
    vmem_bf16(BLOCK, WIDTH),
    vmem_bf16(HEADS, BLOCK, HEAD_DIM),
    vmem_bf16(HEADS, BLOCK, COLUMN * HEAD_DIM),
    vmem_f32(BLOCK, WIDTH),
    vmem_bf16(2, COLUMN, BLOCKS, SLICE, WIDTH),
    vmem_f32(1, TILE_Q),
    vmem_f32(1, TILE_Q),
    vmem_f32(HEAD_DIM, TILE_Q),
    vmem_f32(BLOCK, TILE_Q),
    vmem_f32(BLOCK, TILE_Q),
    DMA((BLOCK // ROWS,)), DMA((2, COLUMN)), DMA((COLS,)),
] + column_sems(HEADS, 2)


def attention_parts(layer, windowed, z, cp, k_buf, v_buf, slot_of, x_ref, wo_ref, full_ref, out_ref,
                    xh, q_buf, o_all, acc, wo_buf, m_s, l_s, a_s, s0, s1, x_sem, wo_sem, out_sem, o_send, o_recv):
    def load_x(i):
        return pltpu.make_async_copy(x_ref.at[rows_of(i), :], xh.at[rows_of(i), :], x_sem.at[i])

    def gather(h, t):
        def part(me, target):
            return o_all.at[h, rows_of(t, TILE_Q), lanes_of(me)]
        return ColumnGather(z, cp, part, part, o_send.at[h, t], o_recv.at[h, t])

    def o_pass(h):
        for t in range(TILES):
            gather(h, t).passing()

    key_iota = lax.broadcasted_iota(jnp.int32, (BLOCK, TILE_Q), 0)
    row_iota = lax.broadcasted_iota(jnp.int32, (BLOCK, TILE_Q), 1)

    @scoped("attend")
    def attend(h, t):
        q = q_buf[h, rows_of(t, TILE_Q), :]
        ks, vs = k_buf.at[slot_of(h)], v_buf.at[slot_of(h)]

        def scores(j):
            return dot_rows(ks[j], q)

        def soft(s, j, first=False):
            m_new = jnp.max(s, axis=0, keepdims=True)
            if not first:
                m_old = m_s[...]
                m_new = jnp.maximum(m_old, m_new)
                alpha = jnp.exp2((m_old - m_new) * EXP_SCALE)
            p = jnp.exp2((s - m_new) * EXP_SCALE)
            norm = jnp.sum(p, axis=0, keepdims=True)
            out = jnp.dot(vs[j], p.astype(BF16), preferred_element_type=F32)
            l_s[...] = norm if first else l_s[...] * alpha + norm
            a_s[...] = out if first else a_s[...] * alpha + out
            m_s[...] = m_new

        lo = jnp.maximum(cp - (WINDOW_BLOCKS - 1), 0) if windowed else 0
        count = cp - lo
        s0[...] = scores(cp)
        s1[...] = scores(jnp.minimum(lo, cp))
        soft(jnp.where(key_iota <= row_iota + t * TILE_Q, s0[...], MASKED), cp, True)

        @loop(0, count // 2)
        def _(i):
            j = lo + 2 * i
            s0[...] = scores(j + 1)
            soft(s1[...], j)
            s1[...] = scores(jnp.minimum(j + 2, cp))
            soft(s0[...], j + 1)

        @pl.when(count % 2 == 1)
        def _():
            soft(s1[...], cp - 1)

        if windowed:
            @pl.when(cp >= WINDOW_BLOCKS)
            def _():
                edge = cp - WINDOW_BLOCKS
                soft(jnp.where(key_iota > row_iota + t * TILE_Q, scores(edge), MASKED), edge)

        o_all[h, rows_of(t, TILE_Q), lanes_of(z)] = (a_s[...] / l_s[...]).T.astype(BF16)

    def load_wo(h, action=start):
        slot = h % 2
        for part in range(COLUMN):
            rel = lax.rem(part - z + COLUMN, COLUMN)

            def load(src):
                action(pltpu.make_async_copy(src, wo_buf.at[slot, part], wo_sem.at[slot, part]))
            pl.when(rel == 0)(lambda: load(wo_ref.at[layer, h]))
            pl.when(rel > 0)(lambda: load(full_ref.at[h, rel - 1]))

    def store_out(i):
        cols = rows_of(i, TILE_Q)
        return pltpu.make_async_copy(xh.at[:, cols], out_ref.at[:, cols], out_sem.at[i])

    @scoped("apply_wo")
    def apply_wo(h):
        for t in range(TILES):
            gather(h, t).finish()
        load_wo(h, wait)

        @pl.when(h == HEADS - 1)
        def _():
            for i in range(BLOCK // ROWS):
                load_x(i).wait()

        @loop(0, COLS)
        def _(i):
            cols = rows_of(i, TILE_Q)
            weight = wo_buf[h % 2, :, :, :, cols].reshape(COLUMN * HEAD_DIM, TILE_Q)
            part = jnp.dot(o_all[h], weight, preferred_element_type=F32)

            @pl.when(h == 0)
            def _():
                acc[:, cols] = part

            @pl.when((h > 0) & (h < HEADS - 1))
            def _():
                acc[:, cols] += part

            @pl.when(h == HEADS - 1)
            def _():
                xh[:, cols] = (xh[:, cols].astype(F32) + (acc[:, cols] + part)).astype(BF16)
                store_out(i).start()

    def start_x():
        for i in range(BLOCK // ROWS):
            load_x(i).start()

    def drain(h):
        for t in range(TILES):
            gather(h, t).drain()

    def settle():
        for i in range(COLS):
            store_out(i).wait()

    return types.SimpleNamespace(
        load_x=load_x, start_x=start_x, attend=attend, o_start=lambda h, t: gather(h, t).begin(), o_pass=scoped("o_pass")(o_pass),
        load_wo=load_wo, apply_wo=apply_wo, drain=drain, settle=settle)


def first_kernel(x_ref, gain_ref, wq_ref, wk_ref, wv_ref, bias_ref, cos_ref, sin_ref, wo_ref,
                 out_ref, k_out, v_out, full_ref, next_ref,
                 w_buf, k_buf, v_buf, v_nat, w_sem, kv_sem, send_sem, recv_sem, *rest):
    z = lax.axis_index("tp")
    cp = lax.axis_index("cp")
    count = len(ATTENTION_SCRATCH)
    xh, q_buf = rest[:2]
    z_send, z_recv, n_send, n_recv, p_send, p_recv = rest[count:]
    slices = weight_slices(0, z, cp, wo_ref, full_ref, z_send, z_recv)
    next_slices = weight_slices(1, z, cp, wo_ref, next_ref, n_send, n_recv)
    weights = weight_exchange(1, z, cp, full_ref, p_send, p_recv)
    kv = PlaneExchange(z, cp, lambda h, part, block: (k_buf, v_buf)[part].at[h, block], send_sem, recv_sem)
    parts = attention_parts(0, False, z, cp, k_buf, v_buf, lambda h: h, x_ref, wo_ref, full_ref, out_ref, *rest[:count])

    def load_w(h, action):
        slot = h % 2
        for i, w in enumerate((wq_ref, wk_ref, wv_ref)):
            action(pltpu.make_async_copy(w.at[0, :, lanes_of(h)], w_buf.at[slot, :, lanes_of(i)], w_sem.at[slot, i]))

    greet_plane(z, cp)
    greet_column(z, cp)
    parts.start_x()
    load_w(0, start)
    arrive(6)
    slices.begin()
    next_slices.begin()
    gain = gain_ref[:1, :].astype(F32)

    @loop(0, BLOCK // ROWS)
    def _(i):
        parts.load_x(i).wait()
        xh[rows_of(i), :] = normalize(xh[rows_of(i), :], gain)

    def caches(h, action):
        action(pltpu.make_async_copy(k_buf.at[h, cp], k_out.at[h], kv_sem.at[h, 0]))
        action(pltpu.make_async_copy(v_nat.at[h], v_out.at[h], kv_sem.at[h, 1]))

    @loop(0, HEADS)
    @scoped("project")
    def _(h):
        @pl.when(h + 1 < HEADS)
        def _():
            load_w(h + 1, start)
        load_w(h, wait)

        @loop(0, TILES)
        def _(i):
            rows = rows_of(i, TILE_Q)
            proj = jnp.dot(xh[rows, :], w_buf[h % 2], preferred_element_type=F32)
            q, k, v = (proj[:, n * HEAD_DIM:(n + 1) * HEAD_DIM] + bias_ref[h, n:n + 1, :].astype(F32) for n in range(3))
            cos = cos_ref[rows, :]
            sin = sin_ref[rows, :]
            q_buf[h, rows, :] = rotate(q, cos, sin)
            k_buf[h, cp, rows, :] = rotate(k, cos, sin)
            v_nat[h, rows, :] = v.astype(BF16)
            v_buf[h, cp, :, rows] = v.T.astype(BF16)

        @pl.when(h == 0)
        def _():
            kv.own(0)

        @pl.when(h == 3)
        def _():
            kv.near(0)
            kv.own(1)
            kv.own(2)
        caches(h, start)

    slices.passing()
    kv.diagonal(0)
    parts.start_x()

    def between(h):
        pl.when(h == 0)(lambda: kv.near(1))
        pl.when(h + 3 < HEADS)(lambda: kv.own(h + 3))

        @pl.when(h == HEADS - 1)
        def _():
            weights.near(0)
            weights.own(2)

    def behind(h):
        pl.when(h == 0)(next_slices.passing)
        pl.when(h + 1 < HEADS)(lambda: kv.diagonal(h + 1))
        pl.when(h + 2 < HEADS)(lambda: kv.near(h + 2))

        @pl.when(h == HEADS - 3)
        def _():
            slices.finish()
            weights.own(0)
            weights.own(1)
        pl.when(h >= 1)(lambda: parts.o_pass(h - 1))

    @loop(0, HEADS * TILES)
    def _(i):
        h, t = i // TILES, i % TILES
        pl.when(t == 0)(lambda: kv.core(h))
        parts.attend(h, t)
        parts.o_start(h, t)
        pl.when(t == 0)(lambda: between(h))
        pl.when(t == TILES - 1)(lambda: behind(h))

    weights.near(1)
    weights.own(3)
    weights.diagonal(0)

    @loop(0, HEADS)
    def _(h):
        weights.core(h)
        parts.load_wo(h)
        pl.when(h + 2 < HEADS)(lambda: weights.near(h + 2))
        pl.when(h == 0)(lambda: weights.own(4))
        pl.when(h == 2)(lambda: parts.o_pass(HEADS - 1))
        pl.when((h >= 1) & (h + 1 < HEADS))(lambda: weights.diagonal(h + 1))
        parts.apply_wo(h)
        pl.when(h == 0)(lambda: weights.diagonal(1))

    @loop(0, HEADS)
    def _(h):
        kv.drain(h)
        weights.drain(h)
        caches(h, wait)
        parts.drain(h)

    next_slices.finish()
    next_slices.drain()
    slices.drain()
    parts.settle()


def first_call(*args):
    return pl.pallas_call(
        first_kernel,
        out_shape=(bf16(BLOCK, WIDTH), bf16(HEADS, BLOCK, HEAD_DIM), bf16(HEADS, BLOCK, HEAD_DIM),
                   bf16(*FULL_SHAPE), bf16(*FULL_SHAPE)),
        in_specs=[hbm(), vmem(), hbm(), hbm(), hbm(), vmem(), vmem(), vmem(), hbm()],
        out_specs=(hbm(),) * 5,
        scratch_shapes=[
            vmem_bf16(2, WIDTH, 3 * HEAD_DIM),
            vmem_bf16(HEADS, BLOCKS, BLOCK, HEAD_DIM),
            vmem_bf16(HEADS, BLOCKS, HEAD_DIM, BLOCK),
            vmem_bf16(HEADS, BLOCK, HEAD_DIM),
            DMA((2, 3)), DMA((HEADS, 2)),
        ] + plane_sems(HEADS) + ATTENTION_SCRATCH + column_sems() + column_sems() + plane_sems(HEADS),
        compiler_params=PARAMS(collective_id=1),
        cost_estimate=cost(7e10),
        name="front0",
    )(*args)


def second_kernel(x_ref, q_ref, k_ref, v_ref, wo_ref, full_ref, out_ref, k_buf, v_buf, q_sem, kv_sem, *rest):
    z = lax.axis_index("tp")
    cp = lax.axis_index("cp")
    parts = attention_parts(
        1, True, z, cp, k_buf, v_buf, lambda h: h % 2, x_ref, wo_ref, full_ref, out_ref, *rest)

    def load_kv(h, action):
        slot = h % 2
        for i, (src, dst) in enumerate(((k_ref, k_buf), (v_ref, v_buf))):
            action(pltpu.make_async_copy(src.at[h], dst.at[slot], kv_sem.at[slot, i]))

    greet_column(z, cp)
    load_q = pltpu.make_async_copy(q_ref, rest[1], q_sem)
    load_q.start()
    load_kv(0, start)
    load_q.wait()
    lag = 2

    def ahead(h):
        load_kv(h, wait)
        pl.when(h + 1 < HEADS)(lambda: load_kv(h + 1, start))

    def behind(h):
        pl.when(h >= 1)(lambda: parts.o_pass(h - 1))

        @pl.when(h >= lag)
        def _():
            parts.load_wo(h - lag + 1)
            parts.apply_wo(h - lag)

    @loop(0, HEADS * TILES)
    def _(i):
        h, t = i // TILES, i % TILES
        pl.when(t == 0)(lambda: ahead(h))
        parts.attend(h, t)

        @pl.when(i == 0)
        def _():
            arrive(3)
            parts.load_wo(0)
            parts.start_x()
        parts.o_start(h, t)
        pl.when(t == TILES - 1)(lambda: behind(h))

    parts.o_pass(HEADS - 1)

    @loop(HEADS - lag, HEADS)
    def _(h):
        @pl.when(h + 1 < HEADS)
        def _():
            parts.load_wo(h + 1)
        parts.apply_wo(h)

    @loop(0, HEADS)
    def _(h):
        parts.drain(h)
    parts.settle()


def second_call(*args):
    return pl.pallas_call(
        second_kernel,
        out_shape=bf16(BLOCK, WIDTH),
        in_specs=[hbm()] * 6,
        out_specs=hbm(),
        scratch_shapes=[
            vmem_bf16(2, BLOCKS, BLOCK, HEAD_DIM),
            vmem_bf16(2, BLOCKS, HEAD_DIM, BLOCK),
            DMA, DMA((2, 2)),
        ] + ATTENTION_SCRATCH,
        compiler_params=PARAMS(collective_id=2),
        cost_estimate=cost(5e10),
        name="front1",
    )(*args)


CHUNKS = BLOCK // CHUNK
HEAD_SLOTS = ((0, 1), (2, 3), (4,), (5,))
PER_CHUNK = CHUNK // PIECE
REGULAR = len(HEAD) + (CHUNKS - 2) * PER_CHUNK


def mlp_kernel(layer, *refs):
    following = layer == 0
    x_ref, gain_ref, wg_ref, wu_ref, wd_ref, *refs = refs
    if following:
        next_gain, wq_ref, wk_ref, wv_ref, bias_ref, cos_ref, sin_ref, _, *refs = refs
        out_ref, q_out, k_out, v_out, k_all, v_all, full_ref, *refs = refs
    else:
        out_ref, *refs = refs
    wg, wu, wd, xv, pv, rv, sv, act, normed, load_sem, r_send, r_recv, s_send, s_recv, x_send, x_recv, x_local, *refs = refs
    z = lax.axis_index("tp")
    cp = lax.axis_index("cp")
    inner = is_middle(z)
    outer = jnp.logical_not(inner)
    partner = z + 1 - 2 * (z % 2)
    middle = jnp.where(inner, 3 - z, z)
    head = [(sum(HEAD[:i]), size, i) for i, size in enumerate(HEAD)]
    tail = [(BLOCK - CHUNK + sum(TAIL[:i]), size, REGULAR + i) for i, size in enumerate(TAIL)]

    parts = [(src.at[layer, cols, :], dst.at[cols, :]) for cols in FFN_PARTS for src, dst in ((wg_ref, wg), (wu_ref, wu))]
    load_x, load_g0, load_u0, load_g1, load_u1, load_d, load_rest = (
        pltpu.make_async_copy(src, dst, load_sem.at[i]) for i, (src, dst) in enumerate((
            (x_ref.at[:CHUNK, :], xv.at[:CHUNK, :]), *parts,
            (wd_ref.at[layer], wd), (x_ref.at[CHUNK:, :], xv.at[CHUNK:, :]))))
    for load in (load_x, load_g0, load_u0):
        load.start()

    signal(partner, cp)
    pl.when(inner)(lambda: signal(middle, cp))
    if following:
        w_buf, q_st, k_st, v_st, n_st, w_sem, st_sem, send_sem, recv_sem, p_send, p_recv = refs
        greet_plane(z, cp)
        weights = weight_exchange(HEADS, z, cp, full_ref, p_send, p_recv)
    pl.when(inner)(lambda: arrive(5 if following else 2))
    pl.when(outer)(lambda: arrive(4 if following else 1))

    gain = gain_ref[layer:layer + 1, :].astype(F32)
    load_x.wait()

    def chunk_rows(j):
        return rows_of(j, CHUNK)

    def piece(i):
        at = CHUNK + (i - len(head)) * PIECE
        return pl.multiple_of(at, PIECE), PIECE, i

    def pieces(j, action):
        def run(parts):
            for part in parts:
                action(part)
        pl.when(j == 0)(lambda: run(head))
        pl.when((j > 0) & (j < CHUNKS - 1))(
            lambda: run([piece(len(head) + (j - 1) * PER_CHUNK + k) for k in range(PER_CHUNK)]))
        pl.when(j == CHUNKS - 1)(lambda: run(tail))

    def piece_copy(src, dst, send, recv, part, dev):
        at, size, i = part
        return remote(src.at[pl.ds(at, size), :], dst.at[pl.ds(at, size), :], send.at[i], recv.at[i], dev, cp)

    def copy_r(part):
        return piece_copy(pv, rv, r_send, r_recv, part, partner)

    def copy_s(part):
        return piece_copy(pv, sv, s_send, s_recv, part, middle)

    def copy_x(part):
        return piece_copy(xv, xv if following else out_ref, x_send, x_recv, part, partner)

    def copy_local(part):
        at, size, i = part
        return pltpu.make_async_copy(xv.at[pl.ds(at, size), :], out_ref.at[pl.ds(at, size), :], x_local.at[i])

    def first(j, waits, *starts):
        @pl.when(j == 0)
        def _():
            waits.wait()
            for load in starts:
                load.start()

    @scoped("activate")
    def activate(j, part):
        cols = FFN_PARTS[part]
        if part:
            first(j, load_g1, load_d, load_rest)
        else:
            normed[...] = normalize(xv[chunk_rows(j), :], gain)
            first(j, load_g0, load_g1, load_u1)
        gate = dot_rows(normed[...], wg[cols, :])
        first(j, load_u1 if part else load_u0)
        up = dot_rows(normed[...], wu[cols, :])
        act[:, cols] = (gate * jax.nn.sigmoid(gate) * up).astype(BF16)

    @scoped("down")
    def down(j):
        pl.when(j == 0)(load_d.wait)
        pl.when(j == 0)(load_rest.wait)
        pv[chunk_rows(j), :] = jnp.dot(act[...], wd[...], preferred_element_type=F32).astype(BF16)

    @scoped("add_end")
    def add_end(part):
        rows = pl.ds(part[0], part[1])
        copy_r(part).wait_recv()
        pv[rows, :] = (pv[rows, :].astype(F32) + rv[rows, :].astype(F32)).astype(BF16)
        copy_s(part).start()

    @scoped("add_middle")
    def add_middle(part):
        rows = pl.ds(part[0], part[1])
        copy_s(part).wait_recv()
        total = pv[rows, :].astype(F32) + sv[rows, :].astype(F32)
        xv[rows, :] = (xv[rows, :].astype(F32) + total).astype(BF16)
        copy_x(part).start()
        copy_local(part).start()

    if following:
        load_w = [
            pltpu.make_async_copy(w.at[layer + 1], w_buf.at[i], w_sem.at[i])
            for i, w in enumerate((wq_ref, wk_ref, wv_ref))]
        gain_n = next_gain[layer + 1:layer + 2, :].astype(F32)

        def kv_ref(c, part, block):
            rows = chunk_rows(c)
            return v_all.at[:, block, :, rows] if part else k_all.at[:, block, rows, :]
        kv = PlaneExchange(z, cp, kv_ref, send_sem, recv_sem, lambda c, part: (k_st, v_st)[part].at[c % 2])

        def stores(c, action):
            rows = chunk_rows(c)
            slot = c % 2
            for i, (src, dst) in enumerate((
                    (q_st, q_out.at[:, rows, :]), (k_st, k_out.at[:, rows, :]), (n_st, v_out.at[:, rows, :]),
                    (k_st, kv_ref(c, 0, cp)), (v_st, kv_ref(c, 1, cp)))):
                action(pltpu.make_async_copy(src.at[slot], dst, st_sem.at[slot, i]))

        @scoped("x_wait")
        def x_wait(c):
            def land(part):
                copy_x(part).wait_recv()
                copy_local(part).start()
            pl.when(outer)(lambda: pieces(c, land))

        def project(c):
            x_wait(c)

            @pl.when(c >= 2)
            def _():
                kv.own(c - 2, wait_send)
                stores(c - 2, wait)

            with jax.named_scope("project"):
                rows = chunk_rows(c)
                slot = c % 2
                hidden = normalize(xv[rows, :], gain_n)
                cos = cos_ref[rows, :]
                sin = sin_ref[rows, :]
                for which in range(3):
                    proj = jnp.dot(hidden, w_buf[which], preferred_element_type=F32)
                    for h in range(HEADS):
                        part = proj[:, h * HEAD_DIM:(h + 1) * HEAD_DIM] + bias_ref[h, which:which + 1, :].astype(F32)
                        if which < 2:
                            (q_st, k_st)[which][slot, h] = rotate(part, cos, sin)
                        else:
                            n_st[slot, h] = part.astype(BF16)
                            v_st[slot, h] = part.T.astype(BF16)
            kv.own(c)
            stores(c, start)
            pl.when(c >= 1)(lambda: kv.near(c - 1))
            pl.when(c >= 2)(lambda: kv.diagonal(c - 2))

    def serve(j, slot):
        @pl.when(inner & (j == 1))
        def _():
            for i in HEAD_SLOTS[slot]:
                add_end(head[i])
                if i >= SKEW:
                    add_middle(head[i - SKEW])

        @pl.when(inner & (j > 1))
        def _():
            i = len(head) + (j - 2) * PER_CHUNK + slot
            add_end(piece(i))
            if slot < SKEW:
                pl.when(j == 2)(lambda: add_middle(head[slot - SKEW]))
                pl.when(j > 2)(lambda: add_middle(piece(i - SKEW)))
            else:
                add_middle(piece(i - SKEW))

    def serve_tail(begin, last):
        for i in range(begin, last):
            if i < len(tail):
                add_end(tail[i])
            if i == 0:
                for k in range(SKEW, 0, -1):
                    add_middle(piece(REGULAR - k))
            elif i >= TAIL_SKEW:
                add_middle(tail[i - TAIL_SKEW])

    tail_end = len(tail) + TAIL_SKEW
    lag = jnp.where(inner, 2, 5)

    @loop(0, CHUNKS)
    def _(j):
        activate(j, 0)
        serve(j, 0)
        activate(j, 1)
        serve(j, 1)
        down(j)
        pl.when(outer)(lambda: pieces(j, lambda part: copy_r(part).start()))
        serve(j, 2)

        if following:
            @pl.when(j == 0)
            def _():
                weights.own(0)
                for copy in load_w:
                    copy.start()

            @pl.when(j == 1)
            def _():
                for copy in load_w:
                    copy.wait()
            pl.when(j == jnp.where(inner, 2, 3))(lambda: weights.near(0))
            pl.when(j == 5)(lambda: weights.diagonal(0))
            pl.when(j == 6)(lambda: weights.core(0))
            pl.when(j >= lag)(lambda: project(j - lag))
        serve(j, 3)

    if following:
        @loop(CHUNKS - lag, CHUNKS)
        def _(c):
            pl.when(inner & (c == CHUNKS - 2))(lambda: serve_tail(0, 1))
            pl.when(inner & (c == CHUNKS - 1))(lambda: serve_tail(1, tail_end))
            project(c)
        kv.near(CHUNKS - 1)
        kv.diagonal(CHUNKS - 2)
        kv.diagonal(CHUNKS - 1)

        @loop(0, CHUNKS)
        def _(c):
            kv.core(c)
            kv.drain(c, False)

            @pl.when(c >= CHUNKS - 2)
            def _():
                kv.own(c, wait_send)
                stores(c, wait)
        weights.drain(0)
    else:
        pl.when(inner)(lambda: serve_tail(0, tail_end))

    def drain(part):
        @pl.when(inner)
        def _():
            copy_s(part).wait_send()
            copy_x(part).wait_send()
            copy_local(part).wait()

        @pl.when(outer)
        def _():
            copy_r(part).wait_send()
            if following:
                copy_local(part).wait()
            else:
                copy_x(part).wait_recv()

    @loop(0, CHUNKS)
    def _(j):
        pieces(j, drain)


def mlp_call(layer, *args):
    outs = [bf16(BLOCK, WIDTH)]
    in_specs = [hbm(), vmem(), hbm(), hbm(), hbm()]
    scratch = [vmem_bf16(FFN, WIDTH)] * 3 + [vmem_bf16(BLOCK, WIDTH)] * 4 + [vmem_bf16(CHUNK, FFN), vmem_bf16(CHUNK, WIDTH), DMA((7,))]
    scratch += [DMA((REGULAR + len(TAIL),))] * 7
    aliases = {}
    if layer == 0:
        outs += [bf16(HEADS, BLOCK, HEAD_DIM)] * 3
        outs += [bf16(HEADS, BLOCKS, BLOCK, HEAD_DIM), bf16(HEADS, BLOCKS, HEAD_DIM, BLOCK), bf16(*FULL_SHAPE)]
        in_specs += [vmem(), hbm(), hbm(), hbm(), vmem(), vmem(), vmem(), hbm()]
        aliases = {len(in_specs) - 1: len(outs) - 1}
        scratch += [vmem_bf16(3, WIDTH, HEADS * HEAD_DIM)] + [vmem_bf16(2, HEADS, CHUNK, HEAD_DIM)] * 4
        scratch += [DMA((3,)), DMA((2, 5))] + plane_sems(CHUNKS) + plane_sems(1)
    return pl.pallas_call(
        functools.partial(mlp_kernel, layer),
        out_shape=tuple(outs),
        in_specs=in_specs,
        out_specs=(hbm(),) * len(outs),
        scratch_shapes=scratch,
        input_output_aliases=aliases,
        compiler_params=PARAMS(collective_id=3 + layer),
        cost_estimate=cost(1e11),
        name=f"mlp{layer}",
    )(*args)


def solution(mesh):
    def local_step(x_in, positions, attn_gain, mlp_gain, w_query, b_query, w_key, b_key, w_value, b_value,
                   w_out, w_gate, w_up, w_down):
        inv_freq = 1.0 / (1000000.0 ** (jnp.arange(0, HEAD_DIM, 2, dtype=F32) / HEAD_DIM))
        angles = positions.astype(F32)[:, None] * inv_freq[None, :]
        cos, sin = jnp.cos(angles), jnp.sin(angles)
        cos = jnp.concatenate([cos, cos], axis=1)
        sin = jnp.concatenate([-sin, sin], axis=1)

        w_gate = jnp.swapaxes(w_gate, 1, 2)
        w_up = jnp.swapaxes(w_up, 1, 2)
        wo = w_out.reshape(2, HEADS, BLOCKS, SLICE, WIDTH)
        bias = [jnp.stack([b.reshape(2, HEADS, HEAD_DIM)[layer] for b in (b_query, b_key, b_value)], axis=1)
                for layer in range(2)]
        hidden, k0, v0, _, full1 = first_call(x_in, attn_gain, w_query, w_key, w_value, bias[0], cos, sin, wo)
        hidden, q, k1, v1, k_all, v_all, full1 = mlp_call(
            0, hidden, mlp_gain, w_gate, w_up, w_down, attn_gain, w_query, w_key, w_value, bias[1], cos, sin, full1)
        hidden = second_call(hidden, q, k_all, v_all, wo, full1)
        hidden, = mlp_call(1, hidden, mlp_gain, w_gate, w_up, w_down)
        return (hidden,) + tuple(jnp.swapaxes(cache, 0, 1) for cache in (k0, v0, k1, v1))

    weight_col = P(None, None, "tp")
    bias_col = P(None, "tp")
    weight_row = P(None, "tp", None)
    replicated = P(None, None)
    cache_spec = P("cp", "tp", None)
    in_specs = (P("cp", None), P("cp"), replicated, replicated, weight_col, bias_col, weight_col, bias_col,
                weight_col, bias_col, weight_row, weight_col, weight_col, weight_row)
    out_specs = (P("cp", None), cache_spec, cache_spec, cache_spec, cache_spec)
    return jax.shard_map(local_step, mesh=mesh, in_specs=in_specs, out_specs=out_specs, check_vma=False)
```

```python
import functools
import types

import jax
import jax.numpy as jnp
from jax import lax
from jax.experimental import pallas as pl
from jax.experimental.pallas import tpu as pltpu
from jax.sharding import PartitionSpec as P

MESH = pl.DeviceIdType.MESH
BF16 = jnp.bfloat16
F32 = jnp.float32
DMA = pltpu.SemaphoreType.DMA
HEAD_DIM = 128
HEADS = 5
BLOCK = 1024
BLOCKS = 8
COLUMN = 4
WIDTH = 2560
FFN = 1728
WINDOW_BLOCKS = 4
CHUNK = 128
SLICE = 16
ROWS = 256
PIECE = 32
SKEW = 2
HEAD = (16, 16, 16, 16, 32, 32)
TAIL = (32, 32, 16, 16, 16, 16)
TAIL_SKEW = 3
TILE_Q = 512
EXP_SCALE = HEAD_DIM ** -0.5 * 1.4426950408889634
MASKED = -1e30
VMEM_LIMIT = 67_043_328
FFN_PARTS = (slice(0, 768), slice(768, FFN))
FULL_SHAPE = (HEADS, COLUMN - 1, BLOCKS, SLICE, WIDTH)
PARAMS = functools.partial(pltpu.CompilerParams, vmem_limit_bytes=VMEM_LIMIT, has_side_effects=True)


def hbm():
    return pl.BlockSpec(memory_space=pl.ANY)


def vmem():
    return pl.BlockSpec(memory_space=pltpu.VMEM)


def bf16(*shape):
    return jax.ShapeDtypeStruct(shape, BF16)


def vmem_bf16(*shape):
    return pltpu.VMEM(shape, BF16)


def vmem_f32(*shape):
    return pltpu.VMEM(shape, F32)


def cost(flops):
    return pl.CostEstimate(flops=int(flops), bytes_accessed=int(5e7), transcendentals=0)


def loop(lo, hi):
    def wrap(body):
        def step(i, carry):
            body(i)
            return carry
        lax.fori_loop(lo, hi, step, 0)
    return wrap


def scoped(name):
    def wrap(fn):
        def inner(*args):
            with jax.named_scope(name):
                return fn(*args)
        return inner
    return wrap


def start(copy):
    copy.start()


def wait(copy):
    copy.wait()


def wait_send(copy):
    copy.wait_send()


def rows_of(i, size=ROWS):
    return pl.ds(pl.multiple_of(i * size, size), size)


def lanes_of(i):
    return rows_of(i, HEAD_DIM)


def dot_rows(a, b):
    return lax.dot_general(a, b, (((1,), (1,)), ((), ())), preferred_element_type=F32)


def normalize(rows, gain):
    rows_f = rows.astype(F32)
    variance = jnp.mean(rows_f * rows_f, axis=-1, keepdims=True)
    return (rows_f * lax.rsqrt(variance + 1e-6) * gain).astype(BF16)


def rotate(part, cos, sin):
    return (part * cos + pltpu.roll(part, HEAD_DIM // 2, 1) * sin).astype(BF16)


def remote(src, dst, send, recv, z, cp):
    return pltpu.make_async_remote_copy(
        src_ref=src, dst_ref=dst, send_sem=send, recv_sem=recv, device_id=(z, cp), device_id_type=MESH)


SENDS_TO = ((1, 2), (0, 2, 3), (3, 1, 0), (2, 1))


def is_middle(z):
    return (z == 1) | (z == 2)


def far_end(z):
    return jnp.where(z == 1, 3, 0)


def other_end(z):
    return jnp.where(z == 1, 0, 3)


def on_each(z, fn):
    for me in range(COLUMN):
        pl.when(z == me)(functools.partial(fn, me))


def plane(cp):
    x_dev = cp + 2 - 4 * ((cp // 2) % 2)
    y_dev = cp + 4 - 8 * (cp // 4)
    c_dev = cp + 1 - 2 * (cp % 2)
    d_dev = x_dev + 4 - 8 * (x_dev // 4)
    return x_dev, y_dev, c_dev, d_dev


def signal(z, cp):
    pl.semaphore_signal(pltpu.get_barrier_semaphore(), inc=1, device_id=(z, cp), device_id_type=MESH)


def arrive(count):
    pl.semaphore_wait(pltpu.get_barrier_semaphore(), count)


def greet_column(z, cp):
    for step in range(1, COLUMN):
        signal(lax.rem(z + step, COLUMN), cp)


def greet_plane(z, cp):
    for other in plane(cp)[:3]:
        signal(z, other)


class ColumnGather:
    def __init__(self, z, cp, part, landing, send, recv):
        self.z, self.cp, self.part, self.landing, self.send, self.recv = z, cp, part, landing, send, recv

    def copy(self, me, target):
        return remote(self.part(me, target), self.landing(me, target), self.send.at[target], self.recv.at[me], target, self.cp)

    def forward(self):
        far, target = far_end(self.z), other_end(self.z)
        return remote(self.landing(far, self.z), self.landing(far, target), self.send.at[COLUMN], self.recv.at[far],
                      target, self.cp)

    def received(self, src):
        ref = self.landing(src, self.z)
        remote(ref, ref, self.send.at[COLUMN], self.recv.at[src], self.z, self.cp).wait_recv()

    def each(self, action):
        def fn(me):
            for target in SENDS_TO[me]:
                action(self.copy(me, target))
        on_each(self.z, fn)

    def begin(self):
        self.each(start)

    def passing(self):
        @pl.when(is_middle(self.z))
        def _():
            self.received(far_end(self.z))
            self.forward().start()

    def finish(self):
        def fn(me):
            for src in range(COLUMN):
                if src != me and not (me in (1, 2) and abs(src - me) == 2):
                    self.received(src)
        on_each(self.z, fn)

    def drain(self):
        self.each(wait_send)

        @pl.when(is_middle(self.z))
        def _():
            self.forward().wait_send()


def column_sems(*lead):
    return [DMA((*lead, COLUMN + 1)), DMA((*lead, COLUMN))]


class PlaneExchange:
    OWN, FROM_X, FROM_Y, FROM_D, COPIES = range(6), range(6, 9), range(9, 12), range(12, 14), 14

    def __init__(self, z, cp, ref, send, recv, own_src=None):
        self.z, self.cp, self.ref, self.send, self.recv = z, cp, ref, send, recv
        self.own_src = own_src or (lambda item, part: ref(item, part, cp))
        x_dev, y_dev, c_dev, d_dev = plane(cp)
        self.routes = [(part, cp, dev) for dev in (x_dev, y_dev, c_dev) for part in range(2)]
        self.routes += [(0, x_dev, y_dev), (0, x_dev, c_dev), (1, x_dev, c_dev)]
        self.routes += [(1, y_dev, x_dev), (0, y_dev, c_dev), (1, y_dev, c_dev)]
        self.routes += [(0, d_dev, c_dev), (1, d_dev, c_dev)]

    def copy(self, item, slot):
        part, block, dev = self.routes[slot]
        dst = self.ref(item, part, block)
        src = self.own_src(item, part) if slot in self.OWN else dst
        return remote(src, dst, self.send.at[item, slot], self.recv.at[item, slot], self.z, dev)

    def group(self, item, slots, action=start):
        for slot in slots:
            action(self.copy(item, slot))

    def arrivals(self, item, slots, block):
        for slot in slots:
            ref = self.ref(item, self.routes[slot][0], block)
            remote(ref, ref, self.send.at[item, slot], self.recv.at[item, slot], self.z, plane(self.cp)[2]).wait_recv()

    def own(self, item, action=start):
        self.group(item, self.OWN, action)

    @scoped("near")
    def near(self, item):
        x_dev, y_dev, _, _ = plane(self.cp)
        self.arrivals(item, self.OWN[:2], x_dev)
        self.group(item, self.FROM_X)
        self.arrivals(item, self.OWN[2:4], y_dev)
        self.group(item, self.FROM_Y)

    @scoped("diagonal")
    def diagonal(self, item):
        d_dev = plane(self.cp)[3]
        for passed, slots in ((self.FROM_X, self.FROM_D[:1]), (self.FROM_Y, self.FROM_D[1:])):
            self.arrivals(item, passed[:1], d_dev)
            self.group(item, slots)

    @scoped("core")
    def core(self, item):
        x_dev, y_dev, c_dev, d_dev = plane(self.cp)
        for slots, block in ((self.OWN[4:], c_dev), (self.FROM_X[1:], self.mate(x_dev)),
                             (self.FROM_Y[1:], self.mate(y_dev)), (self.FROM_D, self.mate(d_dev))):
            self.arrivals(item, slots, block)

    @staticmethod
    def mate(dev):
        return plane(dev)[2]

    def drain(self, item, own=True):
        if own:
            self.own(item, wait_send)
        for slots in (self.FROM_X, self.FROM_Y, self.FROM_D):
            self.group(item, slots, wait_send)


def plane_sems(items):
    return [DMA((items, PlaneExchange.COPIES))] * 2


def weight_slices(layer, z, cp, src, full, send, recv):
    def landing(me, target):
        return full.at[:, lax.rem(me - target + COLUMN, COLUMN) - 1, cp]
    return ColumnGather(z, cp, lambda me, target: src.at[layer, :, cp], landing, send, recv)


def weight_exchange(group, z, cp, full, send, recv):
    half = SLICE // 2

    def ref(item, part, block):
        return full.at[pl.ds(item * group, group), :, block, part * half:(part + 1) * half]
    return PlaneExchange(z, cp, ref, send, recv)


TILES = BLOCK // TILE_Q
COLS = WIDTH // TILE_Q
ATTENTION_SCRATCH = [
    vmem_bf16(BLOCK, WIDTH),
    vmem_bf16(HEADS, BLOCK, HEAD_DIM),
    vmem_bf16(HEADS, BLOCK, COLUMN * HEAD_DIM),
    vmem_f32(BLOCK, WIDTH),
    vmem_bf16(2, COLUMN, BLOCKS, SLICE, WIDTH),
    vmem_f32(1, TILE_Q),
    vmem_f32(1, TILE_Q),
    vmem_f32(HEAD_DIM, TILE_Q),
    vmem_f32(BLOCK, TILE_Q),
    vmem_f32(BLOCK, TILE_Q),
    DMA((BLOCK // ROWS,)), DMA((2, COLUMN)), DMA((COLS,)),
] + column_sems(HEADS, 2)


def attention_parts(layer, windowed, z, cp, k_buf, v_buf, slot_of, x_ref, wo_ref, full_ref, out_ref,
                    xh, q_buf, o_all, acc, wo_buf, m_s, l_s, a_s, s0, s1, x_sem, wo_sem, out_sem, o_send, o_recv):
    def load_x(i):
        return pltpu.make_async_copy(x_ref.at[rows_of(i), :], xh.at[rows_of(i), :], x_sem.at[i])

    def gather(h, t):
        def part(me, target):
            return o_all.at[h, rows_of(t, TILE_Q), lanes_of(me)]
        return ColumnGather(z, cp, part, part, o_send.at[h, t], o_recv.at[h, t])

    def o_pass(h):
        for t in range(TILES):
            gather(h, t).passing()

    key_iota = lax.broadcasted_iota(jnp.int32, (BLOCK, TILE_Q), 0)
    row_iota = lax.broadcasted_iota(jnp.int32, (BLOCK, TILE_Q), 1)

    @scoped("attend")
    def attend(h, t):
        q = q_buf[h, rows_of(t, TILE_Q), :]
        ks, vs = k_buf.at[slot_of(h)], v_buf.at[slot_of(h)]

        def scores(j):
            return dot_rows(ks[j], q)

        def soft(s, j, first=False):
            m_new = jnp.max(s, axis=0, keepdims=True)
            if not first:
                m_old = m_s[...]
                m_new = jnp.maximum(m_old, m_new)
                alpha = jnp.exp2((m_old - m_new) * EXP_SCALE)
            p = jnp.exp2((s - m_new) * EXP_SCALE)
            norm = jnp.sum(p, axis=0, keepdims=True)
            out = jnp.dot(vs[j], p.astype(BF16), preferred_element_type=F32)
            l_s[...] = norm if first else l_s[...] * alpha + norm
            a_s[...] = out if first else a_s[...] * alpha + out
            m_s[...] = m_new

        lo = jnp.maximum(cp - (WINDOW_BLOCKS - 1), 0) if windowed else 0
        count = cp - lo
        s0[...] = scores(cp)
        s1[...] = scores(jnp.minimum(lo, cp))
        soft(jnp.where(key_iota <= row_iota + t * TILE_Q, s0[...], MASKED), cp, True)

        @loop(0, count // 2)
        def _(i):
            j = lo + 2 * i
            s0[...] = scores(j + 1)
            soft(s1[...], j)
            s1[...] = scores(jnp.minimum(j + 2, cp))
            soft(s0[...], j + 1)

        @pl.when(count % 2 == 1)
        def _():
            soft(s1[...], cp - 1)

        if windowed:
            @pl.when(cp >= WINDOW_BLOCKS)
            def _():
                edge = cp - WINDOW_BLOCKS
                soft(jnp.where(key_iota > row_iota + t * TILE_Q, scores(edge), MASKED), edge)

        o_all[h, rows_of(t, TILE_Q), lanes_of(z)] = (a_s[...] / l_s[...]).T.astype(BF16)

    def load_wo(h, action=start):
        slot = h % 2
        for part in range(COLUMN):
            rel = lax.rem(part - z + COLUMN, COLUMN)

            def load(src):
                action(pltpu.make_async_copy(src, wo_buf.at[slot, part], wo_sem.at[slot, part]))
            pl.when(rel == 0)(lambda: load(wo_ref.at[layer, h]))
            pl.when(rel > 0)(lambda: load(full_ref.at[h, rel - 1]))

    def store_out(i):
        cols = rows_of(i, TILE_Q)
        return pltpu.make_async_copy(xh.at[:, cols], out_ref.at[:, cols], out_sem.at[i])

    @scoped("apply_wo")
    def apply_wo(h):
        for t in range(TILES):
            gather(h, t).finish()
        load_wo(h, wait)

        @pl.when(h == HEADS - 1)
        def _():
            for i in range(BLOCK // ROWS):
                load_x(i).wait()

        @loop(0, COLS)
        def _(i):
            cols = rows_of(i, TILE_Q)
            weight = wo_buf[h % 2, :, :, :, cols].reshape(COLUMN * HEAD_DIM, TILE_Q)
            part = jnp.dot(o_all[h], weight, preferred_element_type=F32)

            @pl.when(h == 0)
            def _():
                acc[:, cols] = part

            @pl.when((h > 0) & (h < HEADS - 1))
            def _():
                acc[:, cols] += part

            @pl.when(h == HEADS - 1)
            def _():
                xh[:, cols] = (xh[:, cols].astype(F32) + (acc[:, cols] + part)).astype(BF16)
                store_out(i).start()

    def start_x():
        for i in range(BLOCK // ROWS):
            load_x(i).start()

    def drain(h):
        for t in range(TILES):
            gather(h, t).drain()

    def settle():
        for i in range(COLS):
            store_out(i).wait()

    return types.SimpleNamespace(
        load_x=load_x, start_x=start_x, attend=attend, o_start=lambda h, t: gather(h, t).begin(), o_pass=scoped("o_pass")(o_pass),
        load_wo=load_wo, apply_wo=apply_wo, drain=drain, settle=settle)


def first_kernel(x_ref, gain_ref, wq_ref, wk_ref, wv_ref, bq_ref, bk_ref, bv_ref, cos_ref, sin_ref, wo_ref,
                 out_ref, k_out, v_out, full_ref, next_ref,
                 w_buf, k_buf, v_buf, v_nat, w_sem, kv_sem, send_sem, recv_sem, *rest):
    z = lax.axis_index("tp")
    cp = lax.axis_index("cp")
    count = len(ATTENTION_SCRATCH)
    xh, q_buf = rest[:2]
    z_send, z_recv, n_send, n_recv, p_send, p_recv = rest[count:]
    slices = weight_slices(0, z, cp, wo_ref, full_ref, z_send, z_recv)
    next_slices = weight_slices(1, z, cp, wo_ref, next_ref, n_send, n_recv)
    weights = weight_exchange(1, z, cp, full_ref, p_send, p_recv)
    kv = PlaneExchange(z, cp, lambda h, part, block: (k_buf, v_buf)[part].at[h, block], send_sem, recv_sem)
    parts = attention_parts(0, False, z, cp, k_buf, v_buf, lambda h: h, x_ref, wo_ref, full_ref, out_ref, *rest[:count])

    def load_w(h, action):
        slot = h % 2
        for i, w in enumerate((wq_ref, wk_ref, wv_ref)):
            action(pltpu.make_async_copy(w.at[0, :, lanes_of(h)], w_buf.at[slot, :, lanes_of(i)], w_sem.at[slot, i]))

    greet_plane(z, cp)
    greet_column(z, cp)
    parts.start_x()
    load_w(0, start)
    arrive(6)
    slices.begin()
    next_slices.begin()
    gain = gain_ref[:1, :].astype(F32)

    @loop(0, BLOCK // ROWS)
    def _(i):
        parts.load_x(i).wait()
        xh[rows_of(i), :] = normalize(xh[rows_of(i), :], gain)

    def caches(h, action):
        action(pltpu.make_async_copy(k_buf.at[h, cp], k_out.at[h], kv_sem.at[h, 0]))
        action(pltpu.make_async_copy(v_nat.at[h], v_out.at[h], kv_sem.at[h, 1]))

    @loop(0, HEADS)
    @scoped("project")
    def _(h):
        @pl.when(h + 1 < HEADS)
        def _():
            load_w(h + 1, start)
        load_w(h, wait)

        @loop(0, TILES)
        def _(i):
            rows = rows_of(i, TILE_Q)
            proj = jnp.dot(xh[rows, :], w_buf[h % 2], preferred_element_type=F32)
            q, k, v = (proj[:, n * HEAD_DIM:(n + 1) * HEAD_DIM] + bias[:1, lanes_of(h)].astype(F32)
                       for n, bias in enumerate((bq_ref, bk_ref, bv_ref)))
            cos = cos_ref[rows, :]
            sin = sin_ref[rows, :]
            q_buf[h, rows, :] = rotate(q, cos, sin)
            k_buf[h, cp, rows, :] = rotate(k, cos, sin)
            v_nat[h, rows, :] = v.astype(BF16)
            v_buf[h, cp, :, rows] = v.T.astype(BF16)

        @pl.when(h == 0)
        def _():
            kv.own(0)

        @pl.when(h == 3)
        def _():
            kv.near(0)
            kv.own(1)
            kv.own(2)
        caches(h, start)

    slices.passing()
    kv.diagonal(0)
    parts.start_x()

    def between(h):
        pl.when(h == 0)(lambda: kv.near(1))
        pl.when(h + 3 < HEADS)(lambda: kv.own(h + 3))

        @pl.when(h == HEADS - 1)
        def _():
            weights.near(0)
            weights.own(2)

    def behind(h):
        pl.when(h == 0)(next_slices.passing)
        pl.when(h + 1 < HEADS)(lambda: kv.diagonal(h + 1))
        pl.when(h + 2 < HEADS)(lambda: kv.near(h + 2))

        @pl.when(h == HEADS - 3)
        def _():
            slices.finish()
            weights.own(0)
            weights.own(1)
        pl.when(h >= 1)(lambda: parts.o_pass(h - 1))

    @loop(0, HEADS * TILES)
    def _(i):
        h, t = i // TILES, i % TILES
        pl.when(t == 0)(lambda: kv.core(h))
        parts.attend(h, t)
        parts.o_start(h, t)
        pl.when(t == 0)(lambda: between(h))
        pl.when(t == TILES - 1)(lambda: behind(h))

    weights.near(1)
    weights.own(3)

    @loop(0, HEADS)
    def _(h):
        kv.drain(h)
        caches(h, wait)
    next_slices.finish()
    next_slices.drain()
    slices.drain()
    weights.diagonal(0)

    @loop(0, HEADS)
    def _(h):
        weights.core(h)
        parts.load_wo(h)
        pl.when(h + 2 < HEADS)(lambda: weights.near(h + 2))
        pl.when(h == 0)(lambda: weights.own(4))
        pl.when(h == 2)(lambda: parts.o_pass(HEADS - 1))
        pl.when((h >= 1) & (h + 1 < HEADS))(lambda: weights.diagonal(h + 1))
        parts.apply_wo(h)
        pl.when(h == 0)(lambda: weights.diagonal(1))

    @loop(0, HEADS)
    def _(h):
        weights.drain(h)
        parts.drain(h)
    parts.settle()


def first_call(*args):
    return pl.pallas_call(
        first_kernel,
        out_shape=(bf16(BLOCK, WIDTH), bf16(HEADS, BLOCK, HEAD_DIM), bf16(HEADS, BLOCK, HEAD_DIM),
                   bf16(*FULL_SHAPE), bf16(*FULL_SHAPE)),
        in_specs=[hbm(), vmem(), hbm(), hbm(), hbm()] + [vmem()] * 5 + [hbm()],
        out_specs=(hbm(),) * 5,
        scratch_shapes=[
            vmem_bf16(2, WIDTH, 3 * HEAD_DIM),
            vmem_bf16(HEADS, BLOCKS, BLOCK, HEAD_DIM),
            vmem_bf16(HEADS, BLOCKS, HEAD_DIM, BLOCK),
            vmem_bf16(HEADS, BLOCK, HEAD_DIM),
            DMA((2, 3)), DMA((HEADS, 2)),
        ] + plane_sems(HEADS) + ATTENTION_SCRATCH + column_sems() + column_sems() + plane_sems(HEADS),
        compiler_params=PARAMS(collective_id=1),
        cost_estimate=cost(7e10),
        name="front0",
    )(*args)


def second_kernel(x_ref, q_ref, k_ref, v_ref, wo_ref, full_ref, out_ref, k_buf, v_buf, q_sem, kv_sem, *rest):
    z = lax.axis_index("tp")
    cp = lax.axis_index("cp")
    parts = attention_parts(
        1, True, z, cp, k_buf, v_buf, lambda h: h % 2, x_ref, wo_ref, full_ref, out_ref, *rest)

    def load_kv(h, action):
        slot = h % 2
        for i, (src, dst) in enumerate(((k_ref, k_buf), (v_ref, v_buf))):
            action(pltpu.make_async_copy(src.at[h], dst.at[slot], kv_sem.at[slot, i]))

    greet_column(z, cp)
    load_q = pltpu.make_async_copy(q_ref, rest[1], q_sem)
    load_q.start()
    load_kv(0, start)
    load_q.wait()
    lag = 2

    def ahead(h):
        load_kv(h, wait)
        pl.when(h + 1 < HEADS)(lambda: load_kv(h + 1, start))

    def behind(h):
        pl.when(h >= 1)(lambda: parts.o_pass(h - 1))

        @pl.when(h >= lag)
        def _():
            parts.load_wo(h - lag + 1)
            parts.apply_wo(h - lag)

    @loop(0, HEADS * TILES)
    def _(i):
        h, t = i // TILES, i % TILES
        pl.when(t == 0)(lambda: ahead(h))
        parts.attend(h, t)

        @pl.when(i == 0)
        def _():
            arrive(3)
            parts.load_wo(0)
            parts.start_x()
        parts.o_start(h, t)
        pl.when(t == TILES - 1)(lambda: behind(h))

    parts.o_pass(HEADS - 1)

    @loop(HEADS - lag, HEADS)
    def _(h):
        @pl.when(h + 1 < HEADS)
        def _():
            parts.load_wo(h + 1)
        parts.apply_wo(h)

    @loop(0, HEADS)
    def _(h):
        parts.drain(h)
    parts.settle()


def second_call(*args):
    return pl.pallas_call(
        second_kernel,
        out_shape=bf16(BLOCK, WIDTH),
        in_specs=[hbm()] * 6,
        out_specs=hbm(),
        scratch_shapes=[
            vmem_bf16(2, BLOCKS, BLOCK, HEAD_DIM),
            vmem_bf16(2, BLOCKS, HEAD_DIM, BLOCK),
            DMA, DMA((2, 2)),
        ] + ATTENTION_SCRATCH,
        compiler_params=PARAMS(collective_id=2),
        cost_estimate=cost(5e10),
        name="front1",
    )(*args)


CHUNKS = BLOCK // CHUNK
HEAD_SLOTS = ((0, 1), (2, 3), (4,), (5,))
PER_CHUNK = CHUNK // PIECE
REGULAR = len(HEAD) + (CHUNKS - 2) * PER_CHUNK


def mlp_kernel(layer, *refs):
    following = layer == 0
    x_ref, gain_ref, wg_ref, wu_ref, wd_ref, *refs = refs
    if following:
        next_gain, wq_ref, wk_ref, wv_ref, bq_ref, bk_ref, bv_ref, cos_ref, sin_ref, _, *refs = refs
        out_ref, q_out, k_out, v_out, k_all, v_all, full_ref, *refs = refs
    else:
        out_ref, *refs = refs
    wg, wu, wd, xv, pv, rv, sv, act, normed, load_sem, r_send, r_recv, s_send, s_recv, x_send, x_recv, x_local, *refs = refs
    z = lax.axis_index("tp")
    cp = lax.axis_index("cp")
    inner = is_middle(z)
    outer = jnp.logical_not(inner)
    partner = z + 1 - 2 * (z % 2)
    middle = jnp.where(inner, 3 - z, z)
    head = [(sum(HEAD[:i]), size, i) for i, size in enumerate(HEAD)]
    tail = [(BLOCK - CHUNK + sum(TAIL[:i]), size, REGULAR + i) for i, size in enumerate(TAIL)]

    parts = [(src.at[layer, cols, :], dst.at[cols, :]) for cols in FFN_PARTS for src, dst in ((wg_ref, wg), (wu_ref, wu))]
    load_x, load_g0, load_u0, load_g1, load_u1, load_d, load_rest = (
        pltpu.make_async_copy(src, dst, load_sem.at[i]) for i, (src, dst) in enumerate((
            (x_ref.at[:CHUNK, :], xv.at[:CHUNK, :]), *parts,
            (wd_ref.at[layer], wd), (x_ref.at[CHUNK:, :], xv.at[CHUNK:, :]))))
    for load in (load_x, load_g0, load_u0):
        load.start()

    signal(partner, cp)
    pl.when(inner)(lambda: signal(middle, cp))
    if following:
        w_buf, q_st, k_st, v_st, n_st, w_sem, st_sem, send_sem, recv_sem, p_send, p_recv = refs
        greet_plane(z, cp)
        weights = weight_exchange(HEADS, z, cp, full_ref, p_send, p_recv)
    pl.when(inner)(lambda: arrive(5 if following else 2))
    pl.when(outer)(lambda: arrive(4 if following else 1))

    gain = gain_ref[layer:layer + 1, :].astype(F32)
    load_x.wait()

    def chunk_rows(j):
        return rows_of(j, CHUNK)

    def piece(i):
        at = CHUNK + (i - len(head)) * PIECE
        return pl.multiple_of(at, PIECE), PIECE, i

    def pieces(j, action):
        def run(parts):
            for part in parts:
                action(part)
        pl.when(j == 0)(lambda: run(head))
        pl.when((j > 0) & (j < CHUNKS - 1))(
            lambda: run([piece(len(head) + (j - 1) * PER_CHUNK + k) for k in range(PER_CHUNK)]))
        pl.when(j == CHUNKS - 1)(lambda: run(tail))

    def piece_copy(src, dst, send, recv, part, dev):
        at, size, i = part
        return remote(src.at[pl.ds(at, size), :], dst.at[pl.ds(at, size), :], send.at[i], recv.at[i], dev, cp)

    def copy_r(part):
        return piece_copy(pv, rv, r_send, r_recv, part, partner)

    def copy_s(part):
        return piece_copy(pv, sv, s_send, s_recv, part, middle)

    def copy_x(part):
        return piece_copy(xv, xv if following else out_ref, x_send, x_recv, part, partner)

    def copy_local(part):
        at, size, i = part
        return pltpu.make_async_copy(xv.at[pl.ds(at, size), :], out_ref.at[pl.ds(at, size), :], x_local.at[i])

    def first(j, waits, *starts):
        @pl.when(j == 0)
        def _():
            waits.wait()
            for load in starts:
                load.start()

    @scoped("activate")
    def activate(j, part):
        cols = FFN_PARTS[part]
        if part:
            first(j, load_g1, load_d, load_rest)
        else:
            normed[...] = normalize(xv[chunk_rows(j), :], gain)
            first(j, load_g0, load_g1, load_u1)
        gate = dot_rows(normed[...], wg[cols, :])
        first(j, load_u1 if part else load_u0)
        up = dot_rows(normed[...], wu[cols, :])
        act[:, cols] = (gate * jax.nn.sigmoid(gate) * up).astype(BF16)

    @scoped("down")
    def down(j):
        pl.when(j == 0)(load_d.wait)
        pl.when(j == 0)(load_rest.wait)
        pv[chunk_rows(j), :] = jnp.dot(act[...], wd[...], preferred_element_type=F32).astype(BF16)

    @scoped("add_end")
    def add_end(part):
        rows = pl.ds(part[0], part[1])
        copy_r(part).wait_recv()
        pv[rows, :] = (pv[rows, :].astype(F32) + rv[rows, :].astype(F32)).astype(BF16)
        copy_s(part).start()

    @scoped("add_middle")
    def add_middle(part):
        rows = pl.ds(part[0], part[1])
        copy_s(part).wait_recv()
        total = pv[rows, :].astype(F32) + sv[rows, :].astype(F32)
        xv[rows, :] = (xv[rows, :].astype(F32) + total).astype(BF16)
        copy_x(part).start()
        copy_local(part).start()

    if following:
        load_w = [
            pltpu.make_async_copy(w.at[layer + 1], w_buf.at[i], w_sem.at[i])
            for i, w in enumerate((wq_ref, wk_ref, wv_ref))]
        gain_n = next_gain[layer + 1:layer + 2, :].astype(F32)

        def kv_ref(c, part, block):
            rows = chunk_rows(c)
            return v_all.at[:, block, :, rows] if part else k_all.at[:, block, rows, :]
        kv = PlaneExchange(z, cp, kv_ref, send_sem, recv_sem, lambda c, part: (k_st, v_st)[part].at[c % 2])

        def stores(c, action):
            rows = chunk_rows(c)
            slot = c % 2
            for i, (src, dst) in enumerate((
                    (q_st, q_out.at[:, rows, :]), (k_st, k_out.at[:, rows, :]), (n_st, v_out.at[:, rows, :]),
                    (k_st, kv_ref(c, 0, cp)), (v_st, kv_ref(c, 1, cp)))):
                action(pltpu.make_async_copy(src.at[slot], dst, st_sem.at[slot, i]))

        @scoped("x_wait")
        def x_wait(c):
            def land(part):
                copy_x(part).wait_recv()
                copy_local(part).start()
            pl.when(outer)(lambda: pieces(c, land))

        def project(c):
            x_wait(c)

            @pl.when(c >= 2)
            def _():
                kv.own(c - 2, wait_send)
                stores(c - 2, wait)

            with jax.named_scope("project"):
                rows = chunk_rows(c)
                slot = c % 2
                hidden = normalize(xv[rows, :], gain_n)
                cos = cos_ref[rows, :]
                sin = sin_ref[rows, :]
                for which, bias in enumerate((bq_ref, bk_ref, bv_ref)):
                    proj = jnp.dot(hidden, w_buf[which], preferred_element_type=F32)
                    proj += bias[layer + 1:layer + 2, :].astype(F32)
                    for h in range(HEADS):
                        part = proj[:, h * HEAD_DIM:(h + 1) * HEAD_DIM]
                        if which < 2:
                            (q_st, k_st)[which][slot, h] = rotate(part, cos, sin)
                        else:
                            n_st[slot, h] = part.astype(BF16)
                            v_st[slot, h] = part.T.astype(BF16)
            kv.own(c)
            stores(c, start)
            pl.when(c >= 1)(lambda: kv.near(c - 1))
            pl.when(c >= 2)(lambda: kv.diagonal(c - 2))

    def serve(j, slot):
        @pl.when(inner & (j == 1))
        def _():
            for i in HEAD_SLOTS[slot]:
                add_end(head[i])
                if i >= SKEW:
                    add_middle(head[i - SKEW])

        @pl.when(inner & (j > 1))
        def _():
            i = len(head) + (j - 2) * PER_CHUNK + slot
            add_end(piece(i))
            if slot < SKEW:
                pl.when(j == 2)(lambda: add_middle(head[slot - SKEW]))
                pl.when(j > 2)(lambda: add_middle(piece(i - SKEW)))
            else:
                add_middle(piece(i - SKEW))

    def serve_tail(begin, last):
        for i in range(begin, last):
            if i < len(tail):
                add_end(tail[i])
            if i == 0:
                for k in range(SKEW, 0, -1):
                    add_middle(piece(REGULAR - k))
            elif i >= TAIL_SKEW:
                add_middle(tail[i - TAIL_SKEW])

    def drain(part):
        @pl.when(inner)
        def _():
            copy_s(part).wait_send()
            copy_x(part).wait_send()
            copy_local(part).wait()

        @pl.when(outer)
        def _():
            copy_r(part).wait_send()
            if following:
                copy_local(part).wait()
            else:
                copy_x(part).wait_recv()

    def drain_pieces():
        @loop(0, CHUNKS)
        def _(j):
            pieces(j, drain)

    tail_end = len(tail) + TAIL_SKEW
    lag = jnp.where(inner, 2, 5)

    @loop(0, CHUNKS)
    def _(j):
        activate(j, 0)
        serve(j, 0)
        activate(j, 1)
        serve(j, 1)
        down(j)
        pl.when(outer)(lambda: pieces(j, lambda part: copy_r(part).start()))
        serve(j, 2)

        if following:
            @pl.when(j == 0)
            def _():
                weights.own(0)
                for copy in load_w:
                    copy.start()

            @pl.when(j == 1)
            def _():
                for copy in load_w:
                    copy.wait()
            pl.when(j == jnp.where(inner, 2, 3))(lambda: weights.near(0))
            pl.when(j == 5)(lambda: weights.diagonal(0))
            pl.when(j == 6)(lambda: weights.core(0))
            pl.when(j >= lag)(lambda: project(j - lag))
        serve(j, 3)

    if following:
        @loop(CHUNKS - lag, CHUNKS)
        def _(c):
            pl.when(inner & (c == CHUNKS - 2))(lambda: serve_tail(0, 1))
            pl.when(inner & (c == CHUNKS - 1))(lambda: serve_tail(1, tail_end))
            project(c)

        def settle(lo, hi):
            @loop(lo, hi)
            def _(c):
                kv.core(c)
                kv.drain(c, False)

        settle(0, CHUNKS - 2)
        weights.drain(0)
        drain_pieces()
        kv.near(CHUNKS - 1)
        kv.diagonal(CHUNKS - 2)
        kv.diagonal(CHUNKS - 1)
        for c in (CHUNKS - 2, CHUNKS - 1):
            kv.own(c, wait_send)
            stores(c, wait)
        settle(CHUNKS - 2, CHUNKS)
    else:
        pl.when(inner)(lambda: serve_tail(0, tail_end))
        drain_pieces()


def mlp_call(layer, *args):
    outs = [bf16(BLOCK, WIDTH)]
    in_specs = [hbm(), vmem(), hbm(), hbm(), hbm()]
    scratch = [vmem_bf16(FFN, WIDTH)] * 3 + [vmem_bf16(BLOCK, WIDTH)] * 4 + [vmem_bf16(CHUNK, FFN), vmem_bf16(CHUNK, WIDTH), DMA((7,))]
    scratch += [DMA((REGULAR + len(TAIL),))] * 7
    aliases = {}
    if layer == 0:
        outs += [bf16(HEADS, BLOCK, HEAD_DIM)] * 3
        outs += [bf16(HEADS, BLOCKS, BLOCK, HEAD_DIM), bf16(HEADS, BLOCKS, HEAD_DIM, BLOCK), bf16(*FULL_SHAPE)]
        in_specs += [vmem(), hbm(), hbm(), hbm()] + [vmem()] * 5 + [hbm()]
        aliases = {len(in_specs) - 1: len(outs) - 1}
        scratch += [vmem_bf16(3, WIDTH, HEADS * HEAD_DIM)] + [vmem_bf16(2, HEADS, CHUNK, HEAD_DIM)] * 4
        scratch += [DMA((3,)), DMA((2, 5))] + plane_sems(CHUNKS) + plane_sems(1)
    return pl.pallas_call(
        functools.partial(mlp_kernel, layer),
        out_shape=tuple(outs),
        in_specs=in_specs,
        out_specs=(hbm(),) * len(outs),
        scratch_shapes=scratch,
        input_output_aliases=aliases,
        compiler_params=PARAMS(collective_id=3 + layer),
        cost_estimate=cost(1e11),
        name=f"mlp{layer}",
    )(*args)


def finish_kernel(*refs):
    sources, results, (x_buf, c_buf, in_sem, out_sem) = refs[:5], refs[5:10], refs[10:]
    steps = [(sources[0].at[rows_of(i), :], x_buf.at[rows_of(i), :], results[0].at[rows_of(i), :]) for i in range(BLOCK // ROWS)]
    steps += [(src, c_buf.at[i], dst) for i, (src, dst) in enumerate(zip(sources[1:], results[1:]))]
    loads = [pltpu.make_async_copy(src, buf, in_sem.at[i]) for i, (src, buf, _) in enumerate(steps)]
    stores = [pltpu.make_async_copy(buf, dst, out_sem.at[i]) for i, (_, buf, dst) in enumerate(steps)]
    for load in loads:
        load.start()
    for load, store in zip(loads, stores):
        load.wait()
        store.start()
    for store in stores:
        store.wait()


def finish_call(*args):
    return pl.pallas_call(
        finish_kernel,
        out_shape=tuple(bf16(*arg.shape) for arg in args),
        in_specs=[hbm()] * len(args),
        out_specs=(hbm(),) * len(args),
        scratch_shapes=[vmem_bf16(BLOCK, WIDTH), vmem_bf16(4, HEADS, BLOCK, HEAD_DIM), DMA((8,)), DMA((8,))],
        compiler_params=pltpu.CompilerParams(vmem_limit_bytes=VMEM_LIMIT),
        name="finish",
    )(*args)


def solution(mesh):
    def local_step(x_in, positions, attn_gain, mlp_gain, w_query, b_query, w_key, b_key, w_value, b_value,
                   w_out, w_gate, w_up, w_down):
        inv_freq = 1.0 / (1000000.0 ** (jnp.arange(0, HEAD_DIM, 2, dtype=F32) / HEAD_DIM))
        angles = positions.astype(F32)[:, None] * inv_freq[None, :]
        cos, sin = jnp.cos(angles), jnp.sin(angles)
        cos = jnp.concatenate([cos, cos], axis=1)
        sin = jnp.concatenate([-sin, sin], axis=1)

        w_gate = jnp.swapaxes(w_gate, 1, 2)
        w_up = jnp.swapaxes(w_up, 1, 2)
        wo = w_out.reshape(2, HEADS, BLOCKS, SLICE, WIDTH)
        biases = (b_query, b_key, b_value)
        hidden, k0, v0, _, full1 = first_call(x_in, attn_gain, w_query, w_key, w_value, *biases, cos, sin, wo)
        hidden, q, k1, v1, k_all, v_all, full1 = mlp_call(
            0, hidden, mlp_gain, w_gate, w_up, w_down, attn_gain, w_query, w_key, w_value, *biases, cos, sin, full1)
        hidden = second_call(hidden, q, k_all, v_all, wo, full1)
        hidden, = mlp_call(1, hidden, mlp_gain, w_gate, w_up, w_down)
        hidden, *caches = finish_call(hidden, k0, v0, k1, v1)
        return (hidden,) + tuple(jnp.swapaxes(cache, 0, 1) for cache in caches)

    weight_col = P(None, None, "tp")
    bias_col = P(None, "tp")
    weight_row = P(None, "tp", None)
    replicated = P(None, None)
    cache_spec = P("cp", "tp", None)
    in_specs = (P("cp", None), P("cp"), replicated, replicated, weight_col, bias_col, weight_col, bias_col,
                weight_col, bias_col, weight_row, weight_col, weight_col, weight_row)
    out_specs = (P("cp", None), cache_spec, cache_spec, cache_spec, cache_spec)
    return jax.shard_map(local_step, mesh=mesh, in_specs=in_specs, out_specs=out_specs, check_vma=False)
```
